128 devices in a mesh: tm: 32 (over y, x, core), grp: 4 (over z).
Axes of the slice: x: 4, y: 4, z: 4, core: 2. Of those that a mesh axis runs over, the one named last changes fastest.
Arguments:
- series: float32 [524288, 512], P(('tm', 'grp')), may hold values from -6 to 6
- filter_taps: float32 [33], replicated, may hold values from -1 to 1
- sign_flips: int32 [524288], P(('tm', 'grp')), may hold values from -1 to 1, as said below
- samples: int32 [8192], replicated, may hold values from 0 to 524287, as said below
Outputs:
- sketch: float32 [8192, 512], P(('tm', 'grp'))
- r_factor: float32 [512, 512], replicated
The draws below stay inside these ranges and needn't reach their ends.
Inputs may be any that keep to these rules, and one draw needn't show every extreme that they name: `sign_flips`: each entry is -1 or +1. All distinct; the values of samples modulo 4096 take exactly 4096 distinct values, each by exactly 2 consecutive entries; entries are ordered by their value modulo 4096, then by value.
All inputs are finite; a program needn't handle non-finite values.
Results may differ from the reference program's by a relative error of at most 0.0003.
Values sent between devices are 32-bit elements; how exact they have to be, the bound alone decides.
No kernel may reach another device: no remote copies, remote signals or barrier semaphores. Data moves between devices by JAX's collectives and lax.ppermute only.
A program may use at most 128 MiB of HBM per device.

```python
import jax
import jax.numpy as jnp
from jax import lax

W = 512
TAPS = 33
HALF_TAPS = 16
SAMPLES = 8192
ROWS_DEV = 4096
ROWS = 524288
COPIES = 2
DISTINCT = 4096
N_TM = 32
N_GRP = 4


def draw_sign_flips(key, part):
    coins = jax.random.randint(jax.random.fold_in(key, 11), (ROWS,), 0, 2, dtype=jnp.int32)
    return 2 * coins - 1


def draw_samples(key, part):
    blocks_all = ROWS // ROWS_DEV
    shuffled = jax.random.permutation(jax.random.fold_in(key, 23), ROWS_DEV)
    positions = jnp.sort(shuffled[:DISTINCT]).astype(jnp.int32)
    block_keys = jax.random.split(jax.random.fold_in(key, 37), DISTINCT)

    def choose_blocks(one_key):
        return jnp.sort(jax.random.permutation(one_key, blocks_all)[:COPIES]).astype(jnp.int32)
    owners = jax.vmap(choose_blocks)(block_keys)
    return (owners * ROWS_DEV + positions[:, None]).reshape(SAMPLES).astype(jnp.int32)


def steps_of(own_key, dims, pieces, low, high):
    def one(dim, blocks):
        heights = jax.random.uniform(jax.random.fold_in(jax.random.fold_in(own_key, 6), dim), (blocks,), jnp.float32, low / len(pieces), high / len(pieces))
        return jnp.repeat(jnp.exp(heights), dims[dim] // blocks).reshape((-1,) + (1,) * (len(dims) - dim - 1))

    gain = one(*pieces[0])
    for cut in pieces[1:]:
        gain = gain * one(*cut)
    return gain


def normal_values(own_key, shape, spread, most, pieces=(), kind=jnp.bfloat16):
    factor_of = steps_of(own_key, shape, pieces, -0.22, 0.18) if pieces else 1.0
    result = jax.random.normal(own_key, shape, jnp.float32) * spread * factor_of
    return jnp.minimum(jnp.maximum(result, -most), most).astype(kind)


def setup_inputs(seed: int = 0) -> dict:
    arg_keys = jax.random.split(jax.random.key(seed), 5)
    return {
        "series": normal_values(arg_keys[0], (ROWS, W), 1.0, 6.0, ((0, 128),), jnp.float32),
        "filter_taps": normal_values(arg_keys[1], (TAPS,), TAPS ** -0.5, 1.0, (), jnp.float32),
        "sign_flips": draw_sign_flips(jax.random.fold_in(arg_keys[4], 71), 0),
        "samples": draw_samples(jax.random.fold_in(arg_keys[4], 71), 0),
    }


def bit_count(values, width_bits):
    counted = jnp.zeros_like(values)
    for offset in range(width_bits):
        counted = counted + (values >> offset & 1)
    return counted

def hadamard(order):
    row_ids = jnp.arange(order, dtype=jnp.int32)[:, None]
    col_ids = jnp.arange(order, dtype=jnp.int32)[None, :]
    parity = bit_count(row_ids & col_ids, max(order.bit_length(), 1)) & 1
    return (1 - 2 * parity).astype(jnp.float32)

def local_transform(rows_block):
    length, columns = rows_block.shape
    levels = length.bit_length() - 1
    outer = 2 ** ((levels + 1) // 2)
    inner = length // outer
    layered = rows_block.reshape(outer, inner, columns)
    layered = jnp.einsum('ux,xvw->uvw', hadamard(outer), layered, precision=lax.Precision.HIGHEST)
    layered = jnp.einsum('vy,uyw->uvw', hadamard(inner), layered, precision=lax.Precision.HIGHEST)
    return layered.reshape(length, columns)

def reference(series, filter_taps, sign_flips, samples):
    blocks_all = N_TM * N_GRP
    row_scale = 1.0 / jnp.sqrt(jnp.float32(ROWS))
    width_bits = ROWS.bit_length()

    def step(carry, owner):
        first_row = owner * ROWS_DEV
        head_rows = lax.dynamic_slice_in_dim(series, jnp.maximum(first_row - HALF_TAPS, 0).astype(jnp.int32), HALF_TAPS, 0)
        head_rows = head_rows * (owner > 0).astype(jnp.float32)
        tail_rows = lax.dynamic_slice_in_dim(series, jnp.minimum(first_row + ROWS_DEV, ROWS - HALF_TAPS).astype(jnp.int32), HALF_TAPS, 0)
        tail_rows = tail_rows * (owner < blocks_all - 1).astype(jnp.float32)
        middle = lax.dynamic_slice_in_dim(series, first_row.astype(jnp.int32), ROWS_DEV, 0)
        window = jnp.concatenate([head_rows, middle, tail_rows], axis=0)
        filtered = filter_taps[0] * window[0:ROWS_DEV]
        for offset in range(1, TAPS):
            filtered = filtered + filter_taps[offset] * window[offset:offset + ROWS_DEV]
        flips = lax.dynamic_slice_in_dim(sign_flips, first_row.astype(jnp.int32), ROWS_DEV, 0)
        flipped = filtered * flips.astype(jnp.float32)[:, None]
        mixed = local_transform(flipped)
        local_row = samples % ROWS_DEV
        owner_block = samples // ROWS_DEV
        parity = bit_count(owner_block & owner, width_bits) & 1
        weights = (1 - 2 * parity).astype(jnp.float32) * row_scale
        picked = jnp.take(mixed, local_row, axis=0) * weights[:, None]
        return (carry + picked, None)
    start_sum = jnp.zeros((SAMPLES, W), jnp.float32)
    sketch, _ = lax.scan(step, start_sum, jnp.arange(blocks_all, dtype=jnp.int32))
    gram = lax.dot_general(sketch.astype(jnp.float32), sketch.astype(jnp.float32), (((0,), (0,)), ((), ())), precision=lax.Precision.HIGHEST, preferred_element_type=jnp.float32)
    lower = jnp.linalg.cholesky(gram / SAMPLES)
    return (sketch, lower.T)
```

```python
import functools

import jax
import jax.numpy as jnp
import numpy as np
from jax import lax
from jax.experimental import pallas as pl
from jax.experimental.pallas import tpu as pltpu
from jax.sharding import PartitionSpec as P


F32 = jnp.float32
BF16 = jnp.bfloat16
ROWS_DEV = 4096
COLS = 512
HALF = 16
TAPS = 33
BLK = 256
WIN = BLK + 2 * HALF
ROW_SCALE = float(np.float32(1.0) / np.sqrt(np.float32(524288.0)))
Z0, CB, X0, Y0 = 0, 2, 3, 5
VMEM = pltpu.VMEM
WHOLE = pl.BlockSpec(memory_space=VMEM)
SMEM = pl.BlockSpec(memory_space=pltpu.SMEM)


def np_hadamard(order):
    ids = np.arange(order)
    both = ids[:, None] & ids[None, :]
    parity = np.zeros_like(both)
    for offset in range(order.bit_length()):
        parity ^= both >> offset & 1
    return 1 - 2 * parity


def to_partner(value, axis, delta):
    if axis == "z":
        return lax.ppermute(value, "grp", [(i, i ^ delta) for i in range(4)])
    step = {"c": delta, "x": delta << 1, "y": delta << 3}[axis]
    return lax.ppermute(value, "tm", [(i, i ^ step) for i in range(32)])


def prepare_kernel(ids_ref, taps_ref, samples_ref, band_ref, out_ref, turn_ref):
    for r in range(0, BLK, 32):
        offset = lax.broadcasted_iota(jnp.int32, (32, WIN), 1) - (
            lax.broadcasted_iota(jnp.int32, (32, WIN), 0) + r
        )
        band = jnp.zeros((32, WIN), F32)
        for k in range(TAPS):
            band = jnp.where(offset == k, taps_ref[k], band)
        high = band.astype(BF16)
        low = (band - high.astype(F32)).astype(BF16)
        band_ref[r : r + 32, :] = jnp.concatenate([high, high, low], 1)
    yx, core, z = ids_ref[0], ids_ref[1], ids_ref[2]
    for rel in range(16):
        for h in range(2):
            row = ((yx ^ rel) * 2 + core) * 2 + h
            line = lax.shift_right_logical(samples_ref[pl.ds(row, 1), :], 12).astype(F32)
            turn_ref[rel % 2 * 2 + h] = jnp.broadcast_to(line, (128, 128)).T
            for s in range(2):
                for low in range(2):
                    column = turn_ref[rel % 2 * 2 + h, pl.ds(low * 64 + s, 32, stride=2), :]
                    at = pl.multiple_of((z ^ (2 * h + low)) * 32, 32)
                    out_ref[s, rel, pl.ds(at, 32), :] = column.astype(jnp.int32)


def local_kernel(x_ref, prev_ref, next_ref, band_ref, had_ref, flip_ref, keep_ref, send_ref, mid_ref):
    for b in range(16):
        if b == 0:
            window = jnp.concatenate([prev_ref[...], x_ref[0 : BLK + HALF]], 0)
        elif b == 15:
            window = jnp.concatenate([x_ref[b * BLK - HALF :], next_ref[...]], 0)
        else:
            window = x_ref[b * BLK - HALF : (b + 1) * BLK + HALF]
        high = window.astype(BF16)
        low = (window - high.astype(F32)).astype(BF16)
        stacked = jnp.concatenate([high, low, high], 0)
        filtered = jnp.dot(band_ref[...], stacked, preferred_element_type=F32)
        f_high = filtered.astype(BF16)
        f_low = (filtered - f_high.astype(F32)).astype(BF16)
        signed = had_ref[...] * flip_ref[b : b + 1, :].astype(BF16)
        mid_ref[b] = jnp.dot(
            jnp.concatenate([signed, signed], 1),
            jnp.concatenate([f_high, f_low], 0),
            preferred_element_type=F32,
        )

    def butterflies(r, _):
        at = pl.multiple_of(r * 8, 8)
        vals = [mid_ref[b, pl.ds(at, 8), :] for b in range(16)]
        for half in (8, 4, 2, 1):
            vals = [
                vals[i] + vals[i + half] if not i & half else vals[i - half] - vals[i]
                for i in range(16)
            ]
        return vals, at

    def keep_rows(r, _):
        vals, at = butterflies(r, None)
        for i in range(16):
            keep_ref[i, pl.ds(at, 8), :] = vals[i]
        return 0

    def send_rows(r, _):
        vals, _ = butterflies(r + 16, None)
        at = pl.multiple_of(r * 8, 8)
        for i in range(16):
            send_ref[i, pl.ds(at, 8), :] = vals[i]
        return 0

    lax.fori_loop(0, 16, keep_rows, 0)
    lax.fori_loop(0, 16, send_rows, 0)


def sign_of(owner, bit, width):
    e = (1 - 2 * (lax.shift_right_logical(owner, bit) & 1)).astype(F32)
    return jnp.concatenate([e] * (width // 128), -1) if width > 128 else e


def core_a_kernel(keep_ref, recv_ref, o_ref, *outs):
    for dx in range(4):
        for dz in range(4):
            own, other = keep_ref[0, dx, dz], recv_ref[0, dx, dz]
            for s in range(2):
                e = sign_of(o_ref[s, 0, dx, dz], CB, 256)
                outs[dz][s, 0, dx] = own + e * other


def core_b_kernel(keep_ref, recv_ref, o_ref, *outs):
    for dx in range(4):
        for dz in range(4):
            own, other = keep_ref[0, dx, dz], recv_ref[0, dx, dz]
            for s in range(2):
                e = sign_of(o_ref[s, 0, dx, dz], CB, 256)
                outs[dx][s, 0, dz] = own + e * other


def core_c_kernel(keep_l, recv_l, keep_r, recv_r, o_ref, *outs):
    for dy in range(4):
        for dz in range(4):
            for s in range(2):
                e = sign_of(o_ref[s, dy, 0, dz], CB, 256)
                outs[dy][s, 0, dz, :, 0:256] = keep_l[dy, 0, dz] + e * recv_l[dy, 0, dz]
                outs[dy][s, 0, dz, :, 256:512] = keep_r[dy, 0, dz] + e * recv_r[dy, 0, dz]


def core_stage_half(kernel, keep, recv, owners):
    by_dy = lambda i: (i, 0, 0, 0, 0)
    return pl.pallas_call(
        kernel,
        grid=(4,),
        in_specs=[
            pl.BlockSpec((1, 4, 4, 24, 256), by_dy),
            pl.BlockSpec((1, 4, 4, 24, 256), by_dy),
            pl.BlockSpec((2, 1, 4, 4, 24, 128), lambda i: (0, i, 0, 0, 0, 0)),
        ],
        out_specs=[pl.BlockSpec((2, 1, 4, 24, 256), lambda i: (0, i, 0, 0, 0))] * 4,
        out_shape=[jax.ShapeDtypeStruct((2, 4, 4, 24, 256), F32)] * 4,
    )(keep, recv, owners)


def core_stage_c(keep_l, recv_l, keep_r, recv_r, owners):
    by_dx = pl.BlockSpec((4, 1, 4, 8, 256), lambda i: (0, i, 0, 3, 0))
    return pl.pallas_call(
        core_c_kernel,
        grid=(4,),
        in_specs=[by_dx] * 4
        + [pl.BlockSpec((2, 4, 1, 4, 8, 128), lambda i: (0, 0, i, 0, 3, 0))],
        out_specs=[pl.BlockSpec((2, 1, 4, 8, 512), lambda i: (0, i, 0, 0, 0))] * 4,
        out_shape=[jax.ShapeDtypeStruct((2, 4, 4, 8, 512), F32)] * 4,
    )(keep_l, recv_l, keep_r, recv_r, owners)


def merged(parts, owner, bit):
    width = parts[0].shape[-1]
    e0, e1 = sign_of(owner, bit, width), sign_of(owner, bit + 1, width)
    return (parts[0] + e0 * parts[1]) + e1 * (parts[2] + e0 * parts[3])


def merge_kernel(bit, cut, *refs):
    ins, o_ref, outs = refs[:4], refs[4], refs[5:]
    lead = ins[0].shape[1:-2]
    for s in range(2):
        for at in np.ndindex(*lead):
            value = merged([r[(s, *at)] for r in ins], o_ref[(s, *at)], bit)
            rest = tuple(v for d, v in enumerate(at) if d != cut)
            outs[at[cut]][(s, *rest)] = value


def merge_stage(parts, owners, bit, cut, block, at):
    shape = parts[0].shape
    out = tuple(v for d, v in enumerate(shape) if d != cut + 1)
    whole = lambda dims: pl.BlockSpec(dims, lambda i: (0,) * len(dims))
    return pl.pallas_call(
        functools.partial(merge_kernel, bit, cut),
        grid=(1,),
        in_specs=[whole(shape)] * 4 + [pl.BlockSpec(block, lambda i: at)],
        out_specs=[whole(out)] * 4,
        out_shape=[jax.ShapeDtypeStruct(out, F32)] * 4,
    )(*parts, owners)


def final_kernel(ids_ref, *refs):
    a_in, b_in, c_in = refs[0:4], refs[4:8], refs[8:12]
    o_ref, sketch_ref, keep_ref, send_ref, gram_ref = refs[12:]
    core, z, me = ids_ref[1], ids_ref[2], ids_ref[3]
    halves = []
    for s in range(2):
        owner = o_ref[s]
        parity = owner & me
        parity = parity ^ lax.shift_right_logical(parity, 4)
        parity = parity ^ lax.shift_right_logical(parity, 2)
        parity = parity ^ lax.shift_right_logical(parity, 1)
        factor = (1 - 2 * (parity & 1)).astype(F32) * ROW_SCALE
        left = merged([r[s] for r in a_in], owner[0:24], Y0)
        right = merged([r[s] for r in b_in], owner[0:24], Z0)
        top = jnp.concatenate([left, right], 1)
        low = merged([r[s] for r in c_in], owner[24:32], X0)
        rows = jnp.concatenate([top, low], 0) * jnp.concatenate([factor] * 4, 1)
        sketch_ref[:, s, :] = rows
        halves.append(rows)
    both = jnp.concatenate(halves, 0)
    gram_ref[...] = lax.dot_general(
        both, both, (((0,), (0,)), ((), ())),
        precision=lax.Precision.HIGHEST, preferred_element_type=F32,
    )
    for d in range(4):
        own = pl.multiple_of((core * 4 + (z ^ d)) * 64, 64)
        other = pl.multiple_of(((1 - core) * 4 + (z ^ d)) * 64, 64)
        keep_ref[d] = gram_ref[pl.ds(own, 64), :]
        send_ref[d] = gram_ref[pl.ds(other, 64), :]


def lane(tile, at):
    return jnp.broadcast_to(tile[:, at : at + 1], (8, 128))


def sub(tile, at):
    return jnp.broadcast_to(tile[at : at + 1, :], tile.shape)


def cholesky_kernel(ids_ref, s0, s1, s2, s3, p_ref, out_ref, g_ref):
    core, z = ids_ref[1], ids_ref[2]
    for d, mine in enumerate((s0, s1, s2, s3)):
        own = pl.multiple_of((core * 4 + (z ^ d)) * 64, 64)
        other = pl.multiple_of(((1 - core) * 4 + (z ^ d)) * 64, 64)
        g_ref[pl.ds(own, 64), :] = mine[...] * (1.0 / 8192)
        g_ref[pl.ds(other, 64), :] = p_ref[d] * (1.0 / 8192)
    below = lax.broadcasted_iota(jnp.int32, (8, 128), 0)
    row8 = lax.broadcasted_iota(jnp.int32, (8, COLS), 0)
    col8 = lax.broadcasted_iota(jnp.int32, (8, COLS), 1)

    def block(j, _):
        base = pl.multiple_of(j * 128, 128)
        for p in range(16):
            at = pl.multiple_of(base + 8 * p, 8)
            panel = g_ref[pl.ds(at, 8), :]
            diag = g_ref[pl.ds(at, 8), pl.ds(base, 128)]
            cols = [lane(diag, 8 * p + i) for i in range(8)]
            inverse, pivots = [], jnp.ones((8, 128), F32)
            crow = [[None] * 8 for _ in range(8)]
            prow = []
            for i in range(8):
                pivot = sub(cols[i], i)
                pivots = jnp.where(below == i, pivot, pivots)
                inv = 1.0 / pivot
                inverse.append(inv)
                m = jnp.where(below > i, cols[i] * inv, 0.0)
                for k in range(i + 1, 8):
                    crow[i][k] = sub(cols[k], i)
                    cols[k] = cols[k] - m * crow[i][k]
                line = sub(panel, i)
                prow.append(line)
                panel = panel - jnp.concatenate([m] * 4, 1) * line
            scale = lax.rsqrt(pivots)
            done = panel * jnp.concatenate([scale] * 4, 1)
            out_ref[pl.ds(at, 8), :] = jnp.where(col8 >= row8 + at, done, 0.0)
            for q in range(p + 1, 16):
                qat = pl.multiple_of(base + 8 * q, 8)
                tile = g_ref[pl.ds(qat, 8), :]
                qd = g_ref[pl.ds(qat, 8), pl.ds(base, 128)]
                qc = [lane(qd, 8 * p + i) for i in range(8)]
                for i in range(8):
                    m = qc[i] * inverse[i]
                    for k in range(i + 1, 8):
                        qc[k] = qc[k] - m * crow[i][k]
                    tile = tile - jnp.concatenate([m] * 4, 1) * prow[i]
                g_ref[pl.ds(qat, 8), :] = tile

        @pl.when(j < 3)
        def _():
            rows = out_ref[pl.ds(base, 128), :]
            ids = lax.broadcasted_iota(jnp.int32, (128, COLS), 1)
            rows = jnp.where(ids >= base + 128, rows, 0.0)
            g_ref[...] -= lax.dot_general(
                rows, rows, (((0,), (0,)), ((), ())),
                precision=lax.Precision.HIGHEST, preferred_element_type=F32,
            )

        return 0

    lax.fori_loop(0, 4, block, 0)


def parity_of(values, bits):
    counted = jnp.zeros_like(values)
    for offset in range(bits):
        counted = counted ^ (values >> offset & 1)
    return counted


def spread(parts, axis):
    return [parts[0]] + [to_partner(parts[d], axis, d) for d in (1, 2, 3)]


def summed(value, axis):
    one, two, three = (to_partner(value, axis, d) for d in (1, 2, 3))
    return (value + one) + (two + three)


def on_device(series, filter_taps, sign_flips, samples):
    tm, z = lax.axis_index("tm"), lax.axis_index("grp")
    me = tm * 4 + z
    ids = jnp.stack([tm // 2, tm % 2, z, me]).astype(jnp.int32)

    up = [(i, i + 1) for i in range(127)]
    prev = lax.ppermute(series[ROWS_DEV - HALF :], ("tm", "grp"), up)
    nxt = lax.ppermute(series[:HALF], ("tm", "grp"), [(b, a) for a, b in up])

    had = jnp.asarray(np_hadamard(BLK), BF16)
    times = jnp.arange(ROWS_DEV, dtype=jnp.int32).reshape(16, BLK)
    flips = (sign_flips.reshape(16, BLK) * (1 - 2 * parity_of(times & (me * 32), 12))).astype(F32)

    bands, owners = pl.pallas_call(
        prepare_kernel,
        in_specs=[SMEM, SMEM, WHOLE],
        out_specs=[WHOLE] * 2,
        out_shape=[
            jax.ShapeDtypeStruct((BLK, 3 * WIN), BF16),
            jax.ShapeDtypeStruct((2, 16, 128, 128), jnp.int32),
        ],
        scratch_shapes=[VMEM((4, 128, 128), F32)],
    )(ids, filter_taps, samples.reshape(64, 128))
    owners = owners.reshape(2, 4, 4, 4, 32, 128)

    keeps, recvs = [], []
    for half in range(2):
        cut = lambda i, half=half: (0, half)
        keep, send = pl.pallas_call(
            local_kernel,
            grid=(1,),
            in_specs=[
                pl.BlockSpec((ROWS_DEV, 256), cut),
                pl.BlockSpec((HALF, 256), cut),
                pl.BlockSpec((HALF, 256), cut),
                pl.BlockSpec((BLK, 3 * WIN), lambda i: (0, 0)),
                pl.BlockSpec((BLK, BLK), lambda i: (0, 0)),
                pl.BlockSpec((16, BLK), lambda i: (0, 0)),
            ],
            out_specs=[pl.BlockSpec((16, 128, 256), lambda i: (0, 0, 0))] * 2,
            out_shape=[jax.ShapeDtypeStruct((16, 128, 256), F32)] * 2,
            scratch_shapes=[VMEM((16, BLK, 256), F32)],
        )(series, prev, nxt, bands, had, flips)
        keeps.append(keep.reshape(4, 4, 4, 32, 256))
        recvs.append(to_partner(send, "c", 1).reshape(4, 4, 4, 32, 256))

    a = spread(core_stage_half(core_a_kernel, keeps[0], recvs[0], owners), "z")
    b = spread(core_stage_half(core_b_kernel, keeps[1], recvs[1], owners), "x")
    c = spread(core_stage_c(keeps[0], recvs[0], keeps[1], recvs[1], owners), "y")

    top, low, none = (0,) * 6, (0, 0, 0, 0, 3, 0), None
    a = spread(merge_stage(a, owners, Z0, 1, (2, 4, 4, none, 24, 128), top), "x")
    b = spread(merge_stage(b, owners, X0, 0, (2, 4, none, 4, 24, 128), top), "y")
    c = spread(merge_stage(c, owners, Y0, 1, (2, none, 4, 4, 8, 128), low), "z")

    a = spread(merge_stage(a, owners, X0, 0, (2, 4, none, none, 24, 128), top), "y")
    b = spread(merge_stage(b, owners, Y0, 0, (2, none, none, 4, 24, 128), top), "z")
    c = spread(merge_stage(c, owners, Z0, 0, (2, none, 4, none, 8, 128), low), "x")

    sketch, keep, send = pl.pallas_call(
        final_kernel,
        in_specs=[SMEM] + [WHOLE] * 13,
        out_specs=[WHOLE] * 3,
        out_shape=[
            jax.ShapeDtypeStruct((32, 2, COLS), F32),
            jax.ShapeDtypeStruct((4, 64, COLS), F32),
            jax.ShapeDtypeStruct((4, 64, COLS), F32),
        ],
        scratch_shapes=[VMEM((COLS, COLS), F32)],
    )(ids, *a, *b, *c, owners[:, 0, 0, 0])
    sketch = sketch.reshape(64, COLS)

    held = keep + to_partner(send, "c", 1)
    one, two, three = (to_partner(held[d], "z", d) for d in (1, 2, 3))
    share = (held[0] + one) + (two + three)
    share = summed(share, "x")
    share = summed(share, "y")
    near = [share] + [to_partner(share, "z", d) for d in (1, 2, 3)]
    far = to_partner(jnp.stack(near), "c", 1)

    r_factor = pl.pallas_call(
        cholesky_kernel,
        in_specs=[SMEM] + [WHOLE] * 5,
        out_specs=WHOLE,
        out_shape=jax.ShapeDtypeStruct((COLS, COLS), F32),
        scratch_shapes=[VMEM((COLS, COLS), F32)],
    )(ids, *near, far)
    return (sketch, r_factor)


def solution(mesh):
    return jax.shard_map(
        on_device,
        mesh=mesh,
        in_specs=(P(("tm", "grp"), None), P(), P(("tm", "grp")), P()),
        out_specs=(P(("tm", "grp"), None), P()),
        check_vma=False,
    )
```

```python
import functools

import jax
import jax.numpy as jnp
import numpy as np
from jax import lax
from jax.experimental import pallas as pl
from jax.experimental.pallas import tpu as pltpu
from jax.sharding import PartitionSpec as P


F32 = jnp.float32
BF16 = jnp.bfloat16
ROWS_DEV = 4096
COLS = 512
HALF = 16
TAPS = 33
BLK = 256
WIN = BLK + 2 * HALF
ROW_SCALE = float(np.float32(1.0) / np.sqrt(np.float32(524288.0)))
Z0, CB, X0, Y0 = 0, 2, 3, 5
VMEM = pltpu.VMEM
WHOLE = pl.BlockSpec(memory_space=VMEM)
SMEM = pl.BlockSpec(memory_space=pltpu.SMEM)


def np_hadamard(order):
    ids = np.arange(order)
    both = ids[:, None] & ids[None, :]
    parity = np.zeros_like(both)
    for offset in range(order.bit_length()):
        parity ^= both >> offset & 1
    return 1 - 2 * parity


def to_partner(value, axis, delta):
    if axis == "z":
        return lax.ppermute(value, "grp", [(i, i ^ delta) for i in range(4)])
    step = {"c": delta, "x": delta << 1, "y": delta << 3}[axis]
    return lax.ppermute(value, "tm", [(i, i ^ step) for i in range(32)])


def prepare_kernel(ids_ref, taps_ref, samples_ref, band_ref, out_ref, turn_ref):
    for r in range(0, BLK, 32):
        offset = lax.broadcasted_iota(jnp.int32, (32, WIN), 1) - (
            lax.broadcasted_iota(jnp.int32, (32, WIN), 0) + r
        )
        band = jnp.zeros((32, WIN), F32)
        for k in range(TAPS):
            band = jnp.where(offset == k, taps_ref[k], band)
        high = band.astype(BF16)
        low = (band - high.astype(F32)).astype(BF16)
        band_ref[r : r + 32, :] = jnp.concatenate([high, high, low], 1)
    yx, core, z = ids_ref[0], ids_ref[1], ids_ref[2]
    for rel in range(16):
        for h in range(2):
            row = ((yx ^ rel) * 2 + core) * 2 + h
            line = lax.shift_right_logical(samples_ref[pl.ds(row, 1), :], 12).astype(F32)
            turn_ref[rel % 2 * 2 + h] = jnp.broadcast_to(line, (128, 128)).T
            for s in range(2):
                for low in range(2):
                    column = turn_ref[rel % 2 * 2 + h, pl.ds(low * 64 + s, 32, stride=2), :]
                    at = pl.multiple_of((z ^ (2 * h + low)) * 32, 32)
                    out_ref[s, rel, pl.ds(at, 32), :] = column.astype(jnp.int32)


def local_kernel(x_ref, prev_ref, next_ref, band_ref, had_ref, flip_ref, keep_ref, send_ref, mid_ref):
    for b in range(16):
        if b == 0:
            window = jnp.concatenate([prev_ref[...], x_ref[0 : BLK + HALF]], 0)
        elif b == 15:
            window = jnp.concatenate([x_ref[b * BLK - HALF :], next_ref[...]], 0)
        else:
            window = x_ref[b * BLK - HALF : (b + 1) * BLK + HALF]
        high = window.astype(BF16)
        low = (window - high.astype(F32)).astype(BF16)
        stacked = jnp.concatenate([high, low, high], 0)
        filtered = jnp.dot(band_ref[...], stacked, preferred_element_type=F32)
        f_high = filtered.astype(BF16)
        f_low = (filtered - f_high.astype(F32)).astype(BF16)
        signed = had_ref[...] * flip_ref[b : b + 1, :].astype(BF16)
        mid_ref[b] = jnp.dot(
            jnp.concatenate([signed, signed], 1),
            jnp.concatenate([f_high, f_low], 0),
            preferred_element_type=F32,
        )

    def butterflies(r, _):
        at = pl.multiple_of(r * 8, 8)
        vals = [mid_ref[b, pl.ds(at, 8), :] for b in range(16)]
        for half in (8, 4, 2, 1):
            vals = [
                vals[i] + vals[i + half] if not i & half else vals[i - half] - vals[i]
                for i in range(16)
            ]
        return vals, at

    def keep_rows(r, _):
        vals, at = butterflies(r, None)
        for i in range(16):
            keep_ref[i, pl.ds(at, 8), :] = vals[i]
        return 0

    def send_rows(r, _):
        vals, _ = butterflies(r + 16, None)
        at = pl.multiple_of(r * 8, 8)
        for i in range(16):
            send_ref[i, pl.ds(at, 8), :] = vals[i]
        return 0

    lax.fori_loop(0, 16, keep_rows, 0)
    lax.fori_loop(0, 16, send_rows, 0)


def sign_of(owner, bit, width):
    e = (1 - 2 * (lax.shift_right_logical(owner, bit) & 1)).astype(F32)
    return jnp.concatenate([e] * (width // 128), -1) if width > 128 else e


def core_a_kernel(keep_ref, recv_ref, o_ref, *outs):
    for dx in range(4):
        for dz in range(4):
            own, other = keep_ref[0, dx, dz], recv_ref[0, dx, dz]
            for s in range(2):
                e = sign_of(o_ref[s, 0, dx, dz], CB, 256)
                outs[dz][s, 0, dx] = own + e * other


def core_b_kernel(keep_ref, recv_ref, o_ref, *outs):
    for dx in range(4):
        for dz in range(4):
            own, other = keep_ref[0, dx, dz], recv_ref[0, dx, dz]
            for s in range(2):
                e = sign_of(o_ref[s, 0, dx, dz], CB, 256)
                outs[dx][s, 0, dz] = own + e * other


def core_stage(kernel, keep, recv, owners):
    by_dy = lambda i: (i, 0, 0, 0, 0)
    return pl.pallas_call(
        kernel,
        grid=(4,),
        in_specs=[
            pl.BlockSpec((1, 4, 4, 32, 256), by_dy),
            pl.BlockSpec((1, 4, 4, 32, 256), by_dy),
            pl.BlockSpec((2, 1, 4, 4, 32, 128), lambda i: (0, i, 0, 0, 0, 0)),
        ],
        out_specs=[pl.BlockSpec((2, 1, 4, 32, 256), lambda i: (0, i, 0, 0, 0))] * 4,
        out_shape=[jax.ShapeDtypeStruct((2, 4, 4, 32, 256), F32)] * 4,
    )(keep, recv, owners)


def merged(parts, owner, bit):
    width = parts[0].shape[-1]
    e0, e1 = sign_of(owner, bit, width), sign_of(owner, bit + 1, width)
    return (parts[0] + e0 * parts[1]) + e1 * (parts[2] + e0 * parts[3])


def merge_kernel(bit, cut, *refs):
    ins, o_ref, outs = refs[:4], refs[4], refs[5:]
    lead = ins[0].shape[1:-2]
    for s in range(2):
        for at in np.ndindex(*lead):
            value = merged([r[(s, *at)] for r in ins], o_ref[(s, *at)], bit)
            rest = tuple(v for d, v in enumerate(at) if d != cut)
            outs[at[cut]][(s, *rest)] = value


def merge_stage(parts, owners, bit, cut, block):
    shape = parts[0].shape
    out = tuple(v for d, v in enumerate(shape) if d != cut + 1)
    whole = lambda dims: pl.BlockSpec(dims, lambda i: (0,) * len(dims))
    return pl.pallas_call(
        functools.partial(merge_kernel, bit, cut),
        grid=(1,),
        in_specs=[whole(shape)] * 4 + [pl.BlockSpec(block, lambda i: (0,) * 6)],
        out_specs=[whole(out)] * 4,
        out_shape=[jax.ShapeDtypeStruct(out, F32)] * 4,
    )(*parts, owners)


def final_kernel(ids_ref, *refs):
    a_in, b_in = refs[0:4], refs[4:8]
    o_ref, sketch_ref, keep_ref, send_ref, gram_ref = refs[8:]
    core, z, me = ids_ref[1], ids_ref[2], ids_ref[3]
    halves = []
    for s in range(2):
        owner = o_ref[s]
        parity = owner & me
        parity = parity ^ lax.shift_right_logical(parity, 4)
        parity = parity ^ lax.shift_right_logical(parity, 2)
        parity = parity ^ lax.shift_right_logical(parity, 1)
        factor = (1 - 2 * (parity & 1)).astype(F32) * ROW_SCALE
        left = merged([r[s] for r in a_in], owner, X0)
        right = merged([r[s] for r in b_in], owner, Z0)
        rows = jnp.concatenate([left, right], 1) * jnp.concatenate([factor] * 4, 1)
        sketch_ref[:, s, :] = rows
        halves.append(rows)
    both = jnp.concatenate(halves, 0)
    gram_ref[...] = lax.dot_general(
        both, both, (((0,), (0,)), ((), ())),
        precision=lax.Precision.HIGHEST, preferred_element_type=F32,
    )
    for d in range(4):
        own = pl.multiple_of((core * 4 + (z ^ d)) * 64, 64)
        other = pl.multiple_of(((1 - core) * 4 + (z ^ d)) * 64, 64)
        keep_ref[d] = gram_ref[pl.ds(own, 64), :]
        send_ref[d] = gram_ref[pl.ds(other, 64), :]


def lane(tile, at):
    ids = lax.broadcasted_iota(jnp.int32, (8, 128), 1)
    return jnp.broadcast_to(jnp.sum(jnp.where(ids == at, tile, 0.0), axis=1, keepdims=True), (8, 128))


def sub(tile, at):
    return jnp.broadcast_to(tile[at : at + 1, :], tile.shape)


def wide(tile, width):
    return jnp.concatenate([tile] * (width // 128), 1) if width > 128 else tile


def cholesky_kernel(ids_ref, s0, s1, s2, s3, p_ref, out_ref, g_ref):
    core, z = ids_ref[1], ids_ref[2]
    for d, mine in enumerate((s0, s1, s2, s3)):
        own = pl.multiple_of((core * 4 + (z ^ d)) * 64, 64)
        other = pl.multiple_of(((1 - core) * 4 + (z ^ d)) * 64, 64)
        g_ref[pl.ds(own, 64), :] = mine[...] * (1.0 / 8192)
        g_ref[pl.ds(other, 64), :] = p_ref[d] * (1.0 / 8192)
    below = lax.broadcasted_iota(jnp.int32, (8, 128), 0)
    step = 32
    for base in range(0, COLS, step):
        lead = base // 128 * 128
        off, width = base - lead, COLS - lead
        row8 = lax.broadcasted_iota(jnp.int32, (8, width), 0)
        col8 = lax.broadcasted_iota(jnp.int32, (8, width), 1)
        tiles = [g_ref[base + 8 * p : base + 8 * p + 8, lead:] for p in range(step // 8)]
        done = []
        for p in range(step // 8):
            panel = tiles[p]
            cols = [[lane(t[:, :128], off + 8 * p + i) for i in range(8)] for t in tiles[p:]]
            pivots = jnp.ones((8, 128), F32)
            for i in range(8):
                pivot = sub(cols[0][i], i)
                pivots = jnp.where(below == i, pivot, pivots)
                inverse = 1.0 / pivot
                line = sub(tiles[p], i)
                factors = [c[i] * inverse for c in cols]
                factors[0] = jnp.where(below > i, factors[0], 0.0)
                for k in range(i + 1, 8):
                    row = sub(cols[0][k], i)
                    for n, c in enumerate(cols):
                        c[k] = c[k] - factors[n] * row
                for n, f in enumerate(factors):
                    tiles[p + n] = tiles[p + n] - wide(f, width) * line
            rows = tiles[p] * wide(lax.rsqrt(pivots), width)
            rows = jnp.where(col8 >= row8 + (off + 8 * p), rows, 0.0)
            at = base + 8 * p
            out_ref[at : at + 8, lead:] = rows
            if lead:
                out_ref[at : at + 8, :lead] = jnp.zeros((8, lead), F32)
            done.append(rows)
        after = base + step
        if after < COLS:
            left = after // 128 * 128
            rows = jnp.concatenate(done, 0)[:, left - lead :]
            one = rows.astype(BF16)
            rest = rows - one.astype(F32)
            two = rest.astype(BF16)
            three = (rest - two.astype(F32)).astype(BF16)
            update = lax.dot_general(
                jnp.concatenate([one, one, two, one, three, two], 0),
                jnp.concatenate([one, two, one, three, one, two], 0),
                (((0,), (0,)), ((), ())), preferred_element_type=F32,
            )
            g_ref[after:, left:] -= update[after - left :, :]


def parity_of(values, bits):
    counted = jnp.zeros_like(values)
    for offset in range(bits):
        counted = counted ^ (values >> offset & 1)
    return counted


def spread(parts, axis):
    return [parts[0]] + [to_partner(parts[d], axis, d) for d in (1, 2, 3)]


def summed(value, axis):
    one, two, three = (to_partner(value, axis, d) for d in (1, 2, 3))
    return (value + one) + (two + three)


def on_device(series, filter_taps, sign_flips, samples):
    tm, z = lax.axis_index("tm"), lax.axis_index("grp")
    me = tm * 4 + z
    ids = jnp.stack([tm // 2, tm % 2, z, me]).astype(jnp.int32)

    up = [(i, i + 1) for i in range(127)]
    prev = lax.ppermute(series[ROWS_DEV - HALF :], ("tm", "grp"), up)
    nxt = lax.ppermute(series[:HALF], ("tm", "grp"), [(b, a) for a, b in up])

    had = jnp.asarray(np_hadamard(BLK), BF16)
    times = jnp.arange(ROWS_DEV, dtype=jnp.int32).reshape(16, BLK)
    flips = (sign_flips.reshape(16, BLK) * (1 - 2 * parity_of(times & (me * 32), 12))).astype(F32)

    bands, owners = pl.pallas_call(
        prepare_kernel,
        in_specs=[SMEM, SMEM, WHOLE],
        out_specs=[WHOLE] * 2,
        out_shape=[
            jax.ShapeDtypeStruct((BLK, 3 * WIN), BF16),
            jax.ShapeDtypeStruct((2, 16, 128, 128), jnp.int32),
        ],
        scratch_shapes=[VMEM((4, 128, 128), F32)],
    )(ids, filter_taps, samples.reshape(64, 128))
    owners = owners.reshape(2, 4, 4, 4, 32, 128)

    keeps, recvs = [], []
    for half in range(2):
        cut = lambda i, half=half: (0, half)
        keep, send = pl.pallas_call(
            local_kernel,
            grid=(1,),
            in_specs=[
                pl.BlockSpec((ROWS_DEV, 256), cut),
                pl.BlockSpec((HALF, 256), cut),
                pl.BlockSpec((HALF, 256), cut),
                pl.BlockSpec((BLK, 3 * WIN), lambda i: (0, 0)),
                pl.BlockSpec((BLK, BLK), lambda i: (0, 0)),
                pl.BlockSpec((16, BLK), lambda i: (0, 0)),
            ],
            out_specs=[pl.BlockSpec((16, 128, 256), lambda i: (0, 0, 0))] * 2,
            out_shape=[jax.ShapeDtypeStruct((16, 128, 256), F32)] * 2,
            scratch_shapes=[VMEM((16, BLK, 256), F32)],
        )(series, prev, nxt, bands, had, flips)
        keeps.append(keep.reshape(4, 4, 4, 32, 256))
        recvs.append(to_partner(send, "c", 1).reshape(4, 4, 4, 32, 256))

    a = spread(core_stage(core_a_kernel, keeps[0], recvs[0], owners), "z")
    b = spread(core_stage(core_b_kernel, keeps[1], recvs[1], owners), "x")
    none = None
    a = spread(merge_stage(a, owners, Z0, 0, (2, 4, 4, none, 32, 128)), "y")
    a = spread(merge_stage(a, owners, Y0, 0, (2, none, 4, none, 32, 128)), "x")
    b = spread(merge_stage(b, owners, X0, 0, (2, 4, none, 4, 32, 128)), "y")
    b = spread(merge_stage(b, owners, Y0, 0, (2, none, none, 4, 32, 128)), "z")

    sketch, keep, send = pl.pallas_call(
        final_kernel,
        grid=(1,),
        in_specs=[SMEM] + [WHOLE] * 8
        + [pl.BlockSpec((2, none, none, none, 32, 128), lambda i: (0,) * 6)],
        out_specs=[WHOLE] * 3,
        out_shape=[
            jax.ShapeDtypeStruct((32, 2, COLS), F32),
            jax.ShapeDtypeStruct((4, 64, COLS), F32),
            jax.ShapeDtypeStruct((4, 64, COLS), F32),
        ],
        scratch_shapes=[VMEM((COLS, COLS), F32)],
    )(ids, *a, *b, owners)
    sketch = sketch.reshape(64, COLS)

    held = keep + to_partner(send, "c", 1)
    one, two, three = (to_partner(held[d], "z", d) for d in (1, 2, 3))
    share = (held[0] + one) + (two + three)
    share = summed(share, "x")
    share = summed(share, "y")
    near = [share] + [to_partner(share, "z", d) for d in (1, 2, 3)]
    far = to_partner(jnp.stack(near), "c", 1)

    r_factor = pl.pallas_call(
        cholesky_kernel,
        in_specs=[SMEM] + [WHOLE] * 5,
        out_specs=WHOLE,
        out_shape=jax.ShapeDtypeStruct((COLS, COLS), F32),
        scratch_shapes=[VMEM((COLS, COLS), F32)],
    )(ids, *near, far)
    return (sketch, r_factor)


def solution(mesh):
    return jax.shard_map(
        on_device,
        mesh=mesh,
        in_specs=(P(("tm", "grp"), None), P(), P(("tm", "grp")), P()),
        out_specs=(P(("tm", "grp"), None), P()),
        check_vma=False,
    )
```

```python
import functools

import jax
import jax.numpy as jnp
import numpy as np
from jax import lax
from jax.experimental import pallas as pl
from jax.experimental.pallas import tpu as pltpu
from jax.sharding import PartitionSpec as P


F32 = jnp.float32
BF16 = jnp.bfloat16
ROWS_DEV = 4096
COLS = 512
HALF = 16
TAPS = 33
BLK = 256
WIN = BLK + 2 * HALF
ROW_SCALE = float(np.float32(1.0) / np.sqrt(np.float32(524288.0)))
Z0, CB, X0, Y0 = 0, 2, 3, 5
VMEM = pltpu.VMEM
WHOLE = pl.BlockSpec(memory_space=VMEM)
SMEM = pl.BlockSpec(memory_space=pltpu.SMEM)


def np_hadamard(order):
    ids = np.arange(order)
    both = ids[:, None] & ids[None, :]
    parity = np.zeros_like(both)
    for offset in range(order.bit_length()):
        parity ^= both >> offset & 1
    return 1 - 2 * parity


def to_partner(value, axis, delta):
    if axis == "z":
        return lax.ppermute(value, "grp", [(i, i ^ delta) for i in range(4)])
    step = {"c": delta, "x": delta << 1, "y": delta << 3}[axis]
    return lax.ppermute(value, "tm", [(i, i ^ step) for i in range(32)])


def prepare_kernel(ids_ref, taps_ref, samples_ref, flips_ref, band_ref, out_ref, flip_ref, turn_ref):
    for r in range(0, BLK, 32):
        offset = lax.broadcasted_iota(jnp.int32, (32, WIN), 1) - (
            lax.broadcasted_iota(jnp.int32, (32, WIN), 0) + r
        )
        band = jnp.zeros((32, WIN), F32)
        for k in range(TAPS):
            band = jnp.where(offset == k, taps_ref[k], band)
        high = band.astype(BF16)
        low = (band - high.astype(F32)).astype(BF16)
        band_ref[r : r + 32, :] = jnp.concatenate([high, high, low], 1)
    yx, core, z, me = ids_ref[0], ids_ref[1], ids_ref[2], ids_ref[3]
    times = lax.broadcasted_iota(jnp.int32, (16, 128), 0) * BLK + lax.broadcasted_iota(
        jnp.int32, (16, 128), 1
    )
    for h in range(2):
        both = (times + 128 * h) & (me * 32)
        for shift in (8, 4, 2, 1):
            both = both ^ lax.shift_right_logical(both, shift)
        signs = flips_ref[pl.ds(h, 16, stride=2), :] * (1 - 2 * (both & 1))
        flip_ref[:, 128 * h : 128 * h + 128] = signs.astype(F32)
    for rel in range(16):
        for h in range(2):
            row = ((yx ^ rel) * 2 + core) * 2 + h
            line = lax.shift_right_logical(samples_ref[pl.ds(row, 1), :], 12).astype(F32)
            turn_ref[rel % 2 * 2 + h] = jnp.broadcast_to(line, (128, 128)).T
            for s in range(2):
                for low in range(2):
                    column = turn_ref[rel % 2 * 2 + h, pl.ds(low * 64 + s, 32, stride=2), :]
                    at = pl.multiple_of((z ^ (2 * h + low)) * 32, 32)
                    out_ref[s, rel, pl.ds(at, 32), :] = column.astype(jnp.int32)


def local_kernel(x_ref, prev_ref, next_ref, band_ref, had_ref, flip_ref, keep_ref, send_ref, mid_ref):
    for b in range(16):
        if b == 0:
            window = jnp.concatenate([prev_ref[...], x_ref[0 : BLK + HALF]], 0)
        elif b == 15:
            window = jnp.concatenate([x_ref[b * BLK - HALF :], next_ref[...]], 0)
        else:
            window = x_ref[b * BLK - HALF : (b + 1) * BLK + HALF]
        high = window.astype(BF16)
        low = (window - high.astype(F32)).astype(BF16)
        stacked = jnp.concatenate([high, low, high], 0)
        mid_ref[b] = jnp.dot(band_ref[...], stacked, preferred_element_type=F32)
    for b in range(16):
        filtered = mid_ref[b]
        f_high = filtered.astype(BF16)
        f_low = (filtered - f_high.astype(F32)).astype(BF16)
        signed = had_ref[...] * flip_ref[b : b + 1, :].astype(BF16)
        mid_ref[b] = jnp.dot(
            jnp.concatenate([signed, signed], 1),
            jnp.concatenate([f_high, f_low], 0),
            preferred_element_type=F32,
        )

    def butterflies(r, _):
        at = pl.multiple_of(r * 8, 8)
        vals = [mid_ref[b, pl.ds(at, 8), :] for b in range(16)]
        for half in (8, 4, 2, 1):
            vals = [
                vals[i] + vals[i + half] if not i & half else vals[i - half] - vals[i]
                for i in range(16)
            ]
        return vals, at

    def keep_rows(r, _):
        vals, at = butterflies(r, None)
        for i in range(16):
            keep_ref[i, pl.ds(at, 8), :] = vals[i]
        return 0

    def send_rows(r, _):
        vals, _ = butterflies(r + 16, None)
        at = pl.multiple_of(r * 8, 8)
        for i in range(16):
            send_ref[i, pl.ds(at, 8), :] = vals[i]
        return 0

    lax.fori_loop(0, 16, keep_rows, 0)
    lax.fori_loop(0, 16, send_rows, 0)


def sign_of(owner, bit, width):
    e = (1 - 2 * (lax.shift_right_logical(owner, bit) & 1)).astype(F32)
    return jnp.concatenate([e] * (width // 128), -1) if width > 128 else e


def core_a_kernel(keep_ref, recv_ref, o_ref, *outs):
    for dx in range(4):
        for dz in range(4):
            own, other = keep_ref[0, dx, dz], recv_ref[0, dx, dz]
            for s in range(2):
                e = sign_of(o_ref[s, 0, dx, dz], CB, 256)
                outs[dz][s, 0, dx] = own + e * other


def core_b_kernel(keep_ref, recv_ref, o_ref, *outs):
    for dx in range(4):
        for dz in range(4):
            own, other = keep_ref[0, dx, dz], recv_ref[0, dx, dz]
            for s in range(2):
                e = sign_of(o_ref[s, 0, dx, dz], CB, 256)
                outs[dx][s, 0, dz] = own + e * other


def core_stage(kernel, keep, recv, owners):
    by_dy = lambda i: (i, 0, 0, 0, 0)
    return pl.pallas_call(
        kernel,
        grid=(4,),
        in_specs=[
            pl.BlockSpec((1, 4, 4, 32, 256), by_dy),
            pl.BlockSpec((1, 4, 4, 32, 256), by_dy),
            pl.BlockSpec((2, 1, 4, 4, 32, 128), lambda i: (0, i, 0, 0, 0, 0)),
        ],
        out_specs=[pl.BlockSpec((2, 1, 4, 32, 256), lambda i: (0, i, 0, 0, 0))] * 4,
        out_shape=[jax.ShapeDtypeStruct((2, 4, 4, 32, 256), F32)] * 4,
    )(keep, recv, owners)


def merged(parts, owner, bit):
    width = parts[0].shape[-1]
    e0, e1 = sign_of(owner, bit, width), sign_of(owner, bit + 1, width)
    return (parts[0] + e0 * parts[1]) + e1 * (parts[2] + e0 * parts[3])


def merge_kernel(bit, cut, *refs):
    ins, o_ref, outs = refs[:4], refs[4], refs[5:]
    lead = ins[0].shape[1:-2]
    for s in range(2):
        for at in np.ndindex(*lead):
            value = merged([r[(s, *at)] for r in ins], o_ref[(s, *at)], bit)
            rest = tuple(v for d, v in enumerate(at) if d != cut)
            outs[at[cut]][(s, *rest)] = value


def merge_stage(parts, owners, bit, cut, block):
    shape = parts[0].shape
    out = tuple(v for d, v in enumerate(shape) if d != cut + 1)
    whole = lambda dims: pl.BlockSpec(dims, lambda i: (0,) * len(dims))
    return pl.pallas_call(
        functools.partial(merge_kernel, bit, cut),
        grid=(1,),
        in_specs=[whole(shape)] * 4 + [pl.BlockSpec(block, lambda i: (0,) * 6)],
        out_specs=[whole(out)] * 4,
        out_shape=[jax.ShapeDtypeStruct(out, F32)] * 4,
    )(*parts, owners)


def final_kernel(ids_ref, *refs):
    a_in, b_in = refs[0:4], refs[4:8]
    o_ref, sketch_ref, keep_ref, send_ref, gram_ref = refs[8:]
    core, z, me = ids_ref[1], ids_ref[2], ids_ref[3]
    halves = []
    for s in range(2):
        owner = o_ref[s]
        parity = owner & me
        parity = parity ^ lax.shift_right_logical(parity, 4)
        parity = parity ^ lax.shift_right_logical(parity, 2)
        parity = parity ^ lax.shift_right_logical(parity, 1)
        factor = (1 - 2 * (parity & 1)).astype(F32) * ROW_SCALE
        left = merged([r[s] for r in a_in], owner, X0)
        right = merged([r[s] for r in b_in], owner, Z0)
        rows = jnp.concatenate([left, right], 1) * jnp.concatenate([factor] * 4, 1)
        sketch_ref[:, s, :] = rows
        halves.append(rows)
    both = jnp.concatenate(halves, 0)
    gram_ref[...] = lax.dot_general(
        both, both, (((0,), (0,)), ((), ())),
        precision=lax.Precision.HIGHEST, preferred_element_type=F32,
    )
    for d in range(4):
        for ref, slot in ((keep_ref, core * 4 + (z ^ d)), (send_ref, (1 - core) * 4 + (z ^ d))):
            for t in range(3):
                ref[d, :, 128 * t : 128 * t + 128] = gram_ref[gram_block(slot, t)]


def gram_block(slot, t):
    row = pl.multiple_of(slot * 64, 64)
    col = pl.multiple_of(((slot // 2 + t) & 3) * 128, 128)
    return pl.ds(row, 64), pl.ds(col, 128)


def lane(tile, at):
    ids = lax.broadcasted_iota(jnp.int32, (8, 128), 1)
    return jnp.broadcast_to(jnp.sum(jnp.where(ids == at, tile, 0.0), axis=1, keepdims=True), (8, 128))


def sub(tile, at):
    return jnp.broadcast_to(tile[at : at + 1, :], tile.shape)


def wide(tile, width):
    return jnp.concatenate([tile] * (width // 128), 1) if width > 128 else tile


def cholesky_kernel(ids_ref, s0, s1, s2, s3, p_ref, out_ref, g_ref):
    core, z = ids_ref[1], ids_ref[2]
    for d, mine in enumerate((s0, s1, s2, s3)):
        for t in range(3):
            cut = slice(128 * t, 128 * t + 128)
            g_ref[gram_block(core * 4 + (z ^ d), t)] = mine[:, cut] * (1.0 / 8192)
            g_ref[gram_block((1 - core) * 4 + (z ^ d), t)] = p_ref[d, :, cut] * (1.0 / 8192)
    g_ref[0:128, 384:512] = g_ref[384:512, 0:128].T
    below = lax.broadcasted_iota(jnp.int32, (8, 128), 0)
    step = 32
    for base in range(0, COLS, step):
        lead = base // 128 * 128
        off, width = base - lead, COLS - lead
        row8 = lax.broadcasted_iota(jnp.int32, (8, width), 0)
        col8 = lax.broadcasted_iota(jnp.int32, (8, width), 1)
        tiles = [g_ref[base + 8 * p : base + 8 * p + 8, lead:] for p in range(step // 8)]
        done = []
        for p in range(step // 8):
            panel = tiles[p]
            cols = [[lane(t[:, :128], off + 8 * p + i) for i in range(8)] for t in tiles[p:]]
            pivots = jnp.ones((8, 128), F32)
            for i in range(8):
                pivot = sub(cols[0][i], i)
                pivots = jnp.where(below == i, pivot, pivots)
                inverse = 1.0 / pivot
                line = sub(tiles[p], i)
                factors = [c[i] * inverse for c in cols]
                factors[0] = jnp.where(below > i, factors[0], 0.0)
                for k in range(i + 1, 8):
                    row = sub(cols[0][k], i)
                    for n, c in enumerate(cols):
                        c[k] = c[k] - factors[n] * row
                for n, f in enumerate(factors):
                    tiles[p + n] = tiles[p + n] - wide(f, width) * line
            rows = tiles[p] * wide(lax.rsqrt(pivots), width)
            rows = jnp.where(col8 >= row8 + (off + 8 * p), rows, 0.0)
            at = base + 8 * p
            out_ref[at : at + 8, lead:] = rows
            if lead:
                out_ref[at : at + 8, :lead] = jnp.zeros((8, lead), F32)
            done.append(rows)
        after = base + step
        if after < COLS:
            left = after // 128 * 128
            rows = jnp.concatenate(done, 0)[:, left - lead :]
            one = rows.astype(BF16)
            rest = rows - one.astype(F32)
            two = rest.astype(BF16)
            three = (rest - two.astype(F32)).astype(BF16)
            update = lax.dot_general(
                jnp.concatenate([one, one, two, one, three, two], 0),
                jnp.concatenate([one, two, one, three, one, two], 0),
                (((0,), (0,)), ((), ())), preferred_element_type=F32,
            )
            g_ref[after:, left:] -= update[after - left :, :]


def spread(parts, axis):
    return [parts[0]] + [to_partner(parts[d], axis, d) for d in (1, 2, 3)]


def summed(value, axis):
    one, two, three = (to_partner(value, axis, d) for d in (1, 2, 3))
    return (value + one) + (two + three)


def on_device(series, filter_taps, sign_flips, samples):
    tm, z = lax.axis_index("tm"), lax.axis_index("grp")
    me = tm * 4 + z
    ids = jnp.stack([tm // 2, tm % 2, z, me]).astype(jnp.int32)

    up = [(i, i + 1) for i in range(127)]
    prev = lax.ppermute(series[ROWS_DEV - HALF :], ("tm", "grp"), up)
    nxt = lax.ppermute(series[:HALF], ("tm", "grp"), [(b, a) for a, b in up])

    had = jnp.asarray(np_hadamard(BLK), BF16)
    bands, owners, flips = pl.pallas_call(
        prepare_kernel,
        in_specs=[SMEM, SMEM, WHOLE, WHOLE],
        out_specs=[WHOLE] * 3,
        out_shape=[
            jax.ShapeDtypeStruct((BLK, 3 * WIN), BF16),
            jax.ShapeDtypeStruct((2, 16, 128, 128), jnp.int32),
            jax.ShapeDtypeStruct((16, BLK), F32),
        ],
        scratch_shapes=[VMEM((4, 128, 128), F32)],
    )(ids, filter_taps, samples.reshape(64, 128), sign_flips.reshape(32, 128))
    owners = owners.reshape(2, 4, 4, 4, 32, 128)

    keeps, recvs = [], []
    for half in range(2):
        cut = lambda i, half=half: (0, half)
        keep, send = pl.pallas_call(
            local_kernel,
            grid=(1,),
            in_specs=[
                pl.BlockSpec((ROWS_DEV, 256), cut),
                pl.BlockSpec((HALF, 256), cut),
                pl.BlockSpec((HALF, 256), cut),
                pl.BlockSpec((BLK, 3 * WIN), lambda i: (0, 0)),
                pl.BlockSpec((BLK, BLK), lambda i: (0, 0)),
                pl.BlockSpec((16, BLK), lambda i: (0, 0)),
            ],
            out_specs=[pl.BlockSpec((16, 128, 256), lambda i: (0, 0, 0))] * 2,
            out_shape=[jax.ShapeDtypeStruct((16, 128, 256), F32)] * 2,
            scratch_shapes=[VMEM((16, BLK, 256), F32)],
        )(series, prev, nxt, bands, had, flips)
        keeps.append(keep.reshape(4, 4, 4, 32, 256))
        recvs.append(to_partner(send, "c", 1).reshape(4, 4, 4, 32, 256))

    a = spread(core_stage(core_a_kernel, keeps[0], recvs[0], owners), "z")
    b = spread(core_stage(core_b_kernel, keeps[1], recvs[1], owners), "x")
    none = None
    a = spread(merge_stage(a, owners, Z0, 0, (2, 4, 4, none, 32, 128)), "y")
    a = spread(merge_stage(a, owners, Y0, 0, (2, none, 4, none, 32, 128)), "x")
    b = spread(merge_stage(b, owners, X0, 0, (2, 4, none, 4, 32, 128)), "y")
    b = spread(merge_stage(b, owners, Y0, 0, (2, none, none, 4, 32, 128)), "z")

    sketch, keep, send = pl.pallas_call(
        final_kernel,
        grid=(1,),
        in_specs=[SMEM] + [WHOLE] * 8
        + [pl.BlockSpec((2, none, none, none, 32, 128), lambda i: (0,) * 6)],
        out_specs=[WHOLE] * 3,
        out_shape=[
            jax.ShapeDtypeStruct((32, 2, COLS), F32),
            jax.ShapeDtypeStruct((4, 64, 384), F32),
            jax.ShapeDtypeStruct((4, 64, 384), F32),
        ],
        scratch_shapes=[VMEM((COLS, COLS), F32)],
    )(ids, *a, *b, owners)
    sketch = sketch.reshape(64, COLS)

    held = keep + to_partner(send, "c", 1)
    one, two, three = (to_partner(held[d], "z", d) for d in (1, 2, 3))
    share = (held[0] + one) + (two + three)
    share = summed(share, "x")
    share = summed(share, "y")
    near = [share] + [to_partner(share, "z", d) for d in (1, 2, 3)]
    far = to_partner(jnp.stack(near), "c", 1)

    r_factor = pl.pallas_call(
        cholesky_kernel,
        in_specs=[SMEM] + [WHOLE] * 5,
        out_specs=WHOLE,
        out_shape=jax.ShapeDtypeStruct((COLS, COLS), F32),
        scratch_shapes=[VMEM((COLS, COLS), F32)],
    )(ids, *near, far)
    return (sketch, r_factor)


def solution(mesh):
    return jax.shard_map(
        on_device,
        mesh=mesh,
        in_specs=(P(("tm", "grp"), None), P(), P(("tm", "grp")), P()),
        out_specs=(P(("tm", "grp"), None), P()),
        check_vma=False,
    )
```

```python
import functools

import jax
import jax.numpy as jnp
import numpy as np
from jax import lax
from jax.experimental import pallas as pl
from jax.experimental.pallas import tpu as pltpu
from jax.sharding import PartitionSpec as P


F32 = jnp.float32
BF16 = jnp.bfloat16
ROWS_DEV = 4096
COLS = 512
HALF = 16
TAPS = 33
BLK = 256
WIN = BLK + 2 * HALF
ROW_SCALE = float(np.float32(1.0) / np.sqrt(np.float32(524288.0)))
Z0, CB, X0, Y0 = 0, 2, 3, 5
VMEM = pltpu.VMEM
WHOLE = pl.BlockSpec(memory_space=VMEM)
SMEM = pl.BlockSpec(memory_space=pltpu.SMEM)


def np_hadamard(order):
    ids = np.arange(order)
    both = ids[:, None] & ids[None, :]
    parity = np.zeros_like(both)
    for offset in range(order.bit_length()):
        parity ^= both >> offset & 1
    return 1 - 2 * parity


def to_partner(value, axis, delta):
    if axis == "z":
        return lax.ppermute(value, "grp", [(i, i ^ delta) for i in range(4)])
    step = {"c": delta, "x": delta << 1, "y": delta << 3}[axis]
    return lax.ppermute(value, "tm", [(i, i ^ step) for i in range(32)])


def prepare_kernel(ids_ref, taps_ref, flips_ref, band_ref, flip_ref):
    for r in range(0, BLK, 32):
        offset = lax.broadcasted_iota(jnp.int32, (32, WIN), 1) - (
            lax.broadcasted_iota(jnp.int32, (32, WIN), 0) + r
        )
        band = jnp.zeros((32, WIN), F32)
        for k in range(TAPS):
            band = jnp.where(offset == k, taps_ref[k], band)
        high = band.astype(BF16)
        low = (band - high.astype(F32)).astype(BF16)
        band_ref[r : r + 32, :] = jnp.concatenate([high, high, low], 1)
    times = lax.broadcasted_iota(jnp.int32, (16, 128), 0) * BLK + lax.broadcasted_iota(
        jnp.int32, (16, 128), 1
    )
    for h in range(2):
        both = (times + 128 * h) & (ids_ref[3] * 32)
        for shift in (8, 4, 2, 1):
            both = both ^ lax.shift_right_logical(both, shift)
        signs = flips_ref[pl.ds(h, 16, stride=2), :] * (1 - 2 * (both & 1))
        flip_ref[:, 128 * h : 128 * h + 128] = signs.astype(F32)


def owners_kernel(ids_ref, samples_ref, a_ref, b_ref, turn_ref):
    yx, core, z = ids_ref[0], ids_ref[1], ids_ref[2]

    def turned(block, half, slot):
        line = lax.shift_right_logical(samples_ref[pl.ds(block * 2 + half, 1), :], 12).astype(F32)
        turn_ref[slot] = jnp.broadcast_to(line, (128, 128)).T

    def column(slot, s, low):
        return turn_ref[slot, pl.ds(low * 64 + s, 32, stride=2), :].astype(jnp.int32)

    for y in range(4):
        for c in range(2):
            for x in range(4):
                turned((yx ^ (y * 4 + x)) * 2 + (core ^ c), z // 2, x)
                for s in range(2):
                    a_ref[s, y, x, c] = jnp.where(z % 2 == 1, column(x, s, 1), column(x, s, 0))
            for h in range(2):
                turned((yx ^ (y * 4)) * 2 + (core ^ c), h, 4 + h)
                for s in range(2):
                    for low in range(2):
                        b_ref[s, y, c, z ^ (2 * h + low)] = column(4 + h, s, low)


def local_kernel(by_z, x_ref, prev_ref, next_ref, band_ref, had_ref, flip_ref, *refs):
    outs, mid_ref = refs[:4], refs[4]
    for b in range(16):
        if b == 0:
            window = jnp.concatenate([prev_ref[...], x_ref[0 : BLK + HALF]], 0)
        elif b == 15:
            window = jnp.concatenate([x_ref[b * BLK - HALF :], next_ref[...]], 0)
        else:
            window = x_ref[b * BLK - HALF : (b + 1) * BLK + HALF]
        high = window.astype(BF16)
        low = (window - high.astype(F32)).astype(BF16)
        stacked = jnp.concatenate([high, low, high], 0)
        mid_ref[b] = jnp.dot(band_ref[...], stacked, preferred_element_type=F32)
    for b in range(16):
        filtered = mid_ref[b]
        f_high = filtered.astype(BF16)
        f_low = (filtered - f_high.astype(F32)).astype(BF16)
        signed = had_ref[...] * flip_ref[b : b + 1, :].astype(BF16)
        mid_ref[b] = jnp.dot(
            jnp.concatenate([signed, signed], 1),
            jnp.concatenate([f_high, f_low], 0),
            preferred_element_type=F32,
        )

    def butterflies(at):
        vals = [mid_ref[b, pl.ds(at, 8), :] for b in range(16)]
        for half in (8, 4, 2, 1):
            vals = [
                vals[i] + vals[i + half] if not i & half else vals[i - half] - vals[i]
                for i in range(16)
            ]
        return vals

    def rows_of_z(d, r, _):
        core, part = r // 4, r % 4
        vals = butterflies(pl.multiple_of(core * 128 + d * 32 + part * 8, 8))
        for i in range(16):
            outs[d][i, pl.ds(pl.multiple_of(r * 8, 8), 8), :] = vals[i]
        return 0

    def rows_all(r, _):
        at = pl.multiple_of(r * 8, 8)
        vals = butterflies(at)
        for i in range(16):
            outs[i % 4][i // 4, pl.ds(at, 8), :] = vals[i]
        return 0

    if by_z:
        for d in range(4):
            lax.fori_loop(0, 8, functools.partial(rows_of_z, d), 0)
    else:
        lax.fori_loop(0, 32, rows_all, 0)


def sign_of(owner, bit, width):
    e = (1 - 2 * (lax.shift_right_logical(owner, bit) & 1)).astype(F32)
    return jnp.concatenate([e] * (width // 128), -1) if width > 128 else e


def core_kernel(keep_ref, recv_ref, o_ref, *outs):
    for s in range(2):
        for y in range(4):
            for d in range(4):
                e = sign_of(o_ref[s, y, d], CB, 256)
                outs[y][s, d] = keep_ref[s, y, d] + e * recv_ref[s, y, d]


def core_stage(keep, recv, owners, block):
    whole = pl.BlockSpec(keep.shape, lambda i: (0,) * 5)
    return pl.pallas_call(
        core_kernel,
        grid=(1,),
        in_specs=[whole, whole, pl.BlockSpec(block, lambda i: (0,) * 6)],
        out_specs=[pl.BlockSpec((2, 4, 32, 256), lambda i: (0,) * 4)] * 4,
        out_shape=[jax.ShapeDtypeStruct((2, 4, 32, 256), F32)] * 4,
    )(keep, recv, owners)


def merged(parts, owner, bit):
    width = parts[0].shape[-1]
    e0, e1 = sign_of(owner, bit, width), sign_of(owner, bit + 1, width)
    return (parts[0] + e0 * parts[1]) + e1 * (parts[2] + e0 * parts[3])


def merge_kernel(bit, cut, *refs):
    ins, o_ref, outs = refs[:4], refs[4], refs[5:]
    lead = ins[0].shape[1:-2]
    for s in range(2):
        for at in np.ndindex(*lead):
            value = merged([r[(s, *at)] for r in ins], o_ref[(s, *at)], bit)
            rest = tuple(v for d, v in enumerate(at) if d != cut)
            outs[at[cut]][(s, *rest)] = value


def first_kernel(bit, core_dim, *refs):
    ins, o_ref, outs = refs[:4], refs[4], refs[5:]
    lead = ins[0].shape[1:-2]
    for at in np.ndindex(*lead):
        parts = [r[(0, *at)] for r in ins]
        rest = tuple(v for d, v in enumerate(at) if d != core_dim)
        for s in range(2):
            outs[at[core_dim]][(s, 0, *rest)] = merged(parts, o_ref[(s, 0, *at)], bit)


def first_stage(parts, owners, bit, core_dim):
    lead = parts[0].shape[1:-2]
    return pl.pallas_call(
        functools.partial(first_kernel, bit, core_dim),
        grid=(4,),
        in_specs=[pl.BlockSpec((1, *lead, 32, 256), lambda i: (i, 0, 0, 0, 0))] * 4
        + [pl.BlockSpec((2, 1, *lead, 32, 128), lambda i: (0, i, 0, 0, 0, 0))],
        out_specs=[pl.BlockSpec((2, 1, 4, 32, 256), lambda i: (0, i, 0, 0, 0))] * 2,
        out_shape=[jax.ShapeDtypeStruct((2, 4, 4, 32, 256), F32)] * 2,
    )(*parts, owners)


def merge_stage(parts, owners, bit, cut, block):
    shape = parts[0].shape
    out = tuple(v for d, v in enumerate(shape) if d != cut + 1)
    whole = lambda dims: pl.BlockSpec(dims, lambda i: (0,) * len(dims))
    return pl.pallas_call(
        functools.partial(merge_kernel, bit, cut),
        grid=(1,),
        in_specs=[whole(shape)] * 4 + [pl.BlockSpec(block, lambda i: (0,) * 6)],
        out_specs=[whole(out)] * 4,
        out_shape=[jax.ShapeDtypeStruct(out, F32)] * 4,
    )(*parts, owners)


def final_kernel(ids_ref, *refs):
    a_in, b_in = refs[0:4], refs[4:8]
    o_ref, sketch_ref, keep_ref, send_ref, gram_ref = refs[8:]
    core, z, me = ids_ref[1], ids_ref[2], ids_ref[3]
    halves = []
    for s in range(2):
        owner = o_ref[s]
        parity = owner & me
        parity = parity ^ lax.shift_right_logical(parity, 4)
        parity = parity ^ lax.shift_right_logical(parity, 2)
        parity = parity ^ lax.shift_right_logical(parity, 1)
        factor = (1 - 2 * (parity & 1)).astype(F32) * ROW_SCALE
        left = merged([r[s] for r in a_in], owner, X0)
        right = merged([r[s] for r in b_in], owner, Z0)
        rows = jnp.concatenate([left, right], 1) * jnp.concatenate([factor] * 4, 1)
        sketch_ref[:, s, :] = rows
        halves.append(rows)
    both = jnp.concatenate(halves, 0)
    gram_ref[...] = lax.dot_general(
        both, both, (((0,), (0,)), ((), ())),
        precision=lax.Precision.HIGHEST, preferred_element_type=F32,
    )
    for d in range(4):
        for ref, slot in ((keep_ref, core * 4 + (z ^ d)), (send_ref, (1 - core) * 4 + (z ^ d))):
            for t in range(3):
                ref[d, :, 128 * t : 128 * t + 128] = gram_ref[gram_block(slot, t)]


def gram_block(slot, t):
    row = pl.multiple_of(slot * 64, 64)
    col = pl.multiple_of(((slot // 2 + t) & 3) * 128, 128)
    return pl.ds(row, 64), pl.ds(col, 128)


def lane(tile, at):
    ids = lax.broadcasted_iota(jnp.int32, (8, 128), 1)
    return jnp.broadcast_to(jnp.sum(jnp.where(ids == at, tile, 0.0), axis=1, keepdims=True), (8, 128))


def sub(tile, at):
    return jnp.broadcast_to(tile[at : at + 1, :], tile.shape)


def wide(tile, width):
    return jnp.concatenate([tile] * (width // 128), 1) if width > 128 else tile


def cholesky_kernel(ids_ref, s0, s1, s2, s3, p_ref, out_ref, g_ref):
    core, z = ids_ref[1], ids_ref[2]
    for d, mine in enumerate((s0, s1, s2, s3)):
        for t in range(3):
            cut = slice(128 * t, 128 * t + 128)
            g_ref[gram_block(core * 4 + (z ^ d), t)] = mine[:, cut] * (1.0 / 8192)
            g_ref[gram_block((1 - core) * 4 + (z ^ d), t)] = p_ref[d, :, cut] * (1.0 / 8192)
    g_ref[0:128, 384:512] = g_ref[384:512, 0:128].T
    below = lax.broadcasted_iota(jnp.int32, (8, 128), 0)
    step = 32
    for base in range(0, COLS, step):
        lead = base // 128 * 128
        off, width = base - lead, COLS - lead
        row8 = lax.broadcasted_iota(jnp.int32, (8, width), 0)
        col8 = lax.broadcasted_iota(jnp.int32, (8, width), 1)
        tiles = [g_ref[base + 8 * p : base + 8 * p + 8, lead:] for p in range(step // 8)]
        done = []
        for p in range(step // 8):
            cols = [[lane(t[:, :128], off + 8 * p + i) for i in range(8)] for t in tiles[p:]]
            pivots = jnp.ones((8, 128), F32)
            for i in range(8):
                pivot = sub(cols[0][i], i)
                pivots = jnp.where(below == i, pivot, pivots)
                inverse = 1.0 / pivot
                line = sub(tiles[p], i)
                factors = [c[i] * inverse for c in cols]
                factors[0] = jnp.where(below > i, factors[0], 0.0)
                for k in range(i + 1, 8):
                    row = sub(cols[0][k], i)
                    for n, c in enumerate(cols):
                        c[k] = c[k] - factors[n] * row
                for n, f in enumerate(factors):
                    tiles[p + n] = tiles[p + n] - wide(f, width) * line
            rows = tiles[p] * wide(lax.rsqrt(pivots), width)
            rows = jnp.where(col8 >= row8 + (off + 8 * p), rows, 0.0)
            at = base + 8 * p
            out_ref[at : at + 8, lead:] = rows
            if lead:
                out_ref[at : at + 8, :lead] = jnp.zeros((8, lead), F32)
            done.append(rows)
        after = base + step
        if after < COLS:
            left = after // 128 * 128
            rows = jnp.concatenate(done, 0)[:, left - lead :]
            one = rows.astype(BF16)
            rest = rows - one.astype(F32)
            two = rest.astype(BF16)
            three = (rest - two.astype(F32)).astype(BF16)
            update = lax.dot_general(
                jnp.concatenate([one, one, two, one, three, two], 0),
                jnp.concatenate([one, two, one, three, one, two], 0),
                (((0,), (0,)), ((), ())), preferred_element_type=F32,
            )
            g_ref[after:, left:] -= update[after - left :, :]


def spread(parts, axis):
    moved = [parts[0]]
    for d in (1, 2, 3):
        moved.append(to_partner(parts[d], axis, d))
    return moved


def summed(value, axis):
    one, two, three = (to_partner(value, axis, d) for d in (1, 2, 3))
    return (value + one) + (two + three)


def on_device(series, filter_taps, sign_flips, samples):
    tm, z = lax.axis_index("tm"), lax.axis_index("grp")
    me = tm * 4 + z
    ids = jnp.stack([tm // 2, tm % 2, z, me]).astype(jnp.int32)

    up = [(i, i + 1) for i in range(127)]
    prev = lax.ppermute(series[ROWS_DEV - HALF :], ("tm", "grp"), up)
    nxt = lax.ppermute(series[:HALF], ("tm", "grp"), [(b, a) for a, b in up])

    had = jnp.asarray(np_hadamard(BLK), BF16)
    bands, flips = pl.pallas_call(
        prepare_kernel,
        in_specs=[SMEM, SMEM, WHOLE],
        out_specs=[WHOLE] * 2,
        out_shape=[
            jax.ShapeDtypeStruct((BLK, 3 * WIN), BF16),
            jax.ShapeDtypeStruct((16, BLK), F32),
        ],
    )(ids, filter_taps, sign_flips.reshape(32, 128))

    firsts = []
    for half in range(2):
        cut = lambda i, half=half: (0, half)
        out = (16, 64, 256) if half == 0 else (4, 256, 256)
        parts = pl.pallas_call(
            functools.partial(local_kernel, half == 0),
            grid=(1,),
            in_specs=[
                pl.BlockSpec((ROWS_DEV, 256), cut),
                pl.BlockSpec((HALF, 256), cut),
                pl.BlockSpec((HALF, 256), cut),
                pl.BlockSpec((BLK, 3 * WIN), lambda i: (0, 0)),
                pl.BlockSpec((BLK, BLK), lambda i: (0, 0)),
                pl.BlockSpec((16, BLK), lambda i: (0, 0)),
            ],
            out_specs=[pl.BlockSpec(out, lambda i: (0, 0, 0))] * 4,
            out_shape=[jax.ShapeDtypeStruct(out, F32)] * 4,
            scratch_shapes=[VMEM((16, BLK, 256), F32)],
        )(series, prev, nxt, bands, had, flips)
        shape = (4, 4, 2, 32, 256) if half == 0 else (4, 2, 4, 32, 256)
        firsts.append([p.reshape(shape) for p in parts])

    a = spread(firsts[0], "z")
    b = spread(firsts[1], "x")
    late, b[0] = lax.optimization_barrier((samples.reshape(64, 128), b[0]))
    owners_a, owners_b = pl.pallas_call(
        owners_kernel,
        in_specs=[SMEM, WHOLE],
        out_specs=[WHOLE] * 2,
        out_shape=[
            jax.ShapeDtypeStruct((2, 4, 4, 2, 32, 128), jnp.int32),
            jax.ShapeDtypeStruct((2, 4, 2, 4, 32, 128), jnp.int32),
        ],
        scratch_shapes=[VMEM((6, 128, 128), F32)],
    )(ids, late)

    none = None
    keep, send = first_stage(a, owners_a, Z0, 1)
    a = list(core_stage(keep, to_partner(send, "c", 1), owners_a, (2, 4, 4, none, 32, 128)))
    a = spread(a, "y")
    keep, send = first_stage(b, owners_b, X0, 0)
    b = core_stage(keep, to_partner(send, "c", 1), owners_b, (2, 4, none, 4, 32, 128))
    b = spread(b, "y")
    a = merge_stage(a, owners_a, Y0, 0, (2, none, 4, none, 32, 128))
    a = spread(a, "x")
    b = merge_stage(b, owners_b, Y0, 0, (2, none, none, 4, 32, 128))
    b = spread(b, "z")

    sketch, keep, send = pl.pallas_call(
        final_kernel,
        grid=(1,),
        in_specs=[SMEM] + [WHOLE] * 8
        + [pl.BlockSpec((2, none, none, none, 32, 128), lambda i: (0,) * 6)],
        out_specs=[WHOLE] * 3,
        out_shape=[
            jax.ShapeDtypeStruct((32, 2, COLS), F32),
            jax.ShapeDtypeStruct((4, 64, 384), F32),
            jax.ShapeDtypeStruct((4, 64, 384), F32),
        ],
        scratch_shapes=[VMEM((COLS, COLS), F32)],
    )(ids, *a, *b, owners_a)
    sketch = sketch.reshape(64, COLS)

    held = keep + to_partner(send, "c", 1)
    one, two, three = (to_partner(held[d], "z", d) for d in (1, 2, 3))
    share = (held[0] + one) + (two + three)
    share = summed(share, "x")
    share = summed(share, "y")
    near = [share] + [to_partner(share, "z", d) for d in (1, 2, 3)]
    far = to_partner(jnp.stack(near), "c", 1)

    r_factor = pl.pallas_call(
        cholesky_kernel,
        in_specs=[SMEM] + [WHOLE] * 5,
        out_specs=WHOLE,
        out_shape=jax.ShapeDtypeStruct((COLS, COLS), F32),
        scratch_shapes=[VMEM((COLS, COLS), F32)],
    )(ids, *near, far)
    return (sketch, r_factor)


def solution(mesh):
    return jax.shard_map(
        on_device,
        mesh=mesh,
        in_specs=(P(("tm", "grp"), None), P(), P(("tm", "grp")), P()),
        out_specs=(P(("tm", "grp"), None), P()),
        check_vma=False,
    )
```

```python
import functools

import jax
import jax.numpy as jnp
import numpy as np
from jax import lax
from jax.experimental import pallas as pl
from jax.experimental.pallas import tpu as pltpu
from jax.sharding import PartitionSpec as P


F32 = jnp.float32
BF16 = jnp.bfloat16
ROWS_DEV = 4096
COLS = 512
HALF = 16
TAPS = 33
BLK = 256
WIN = BLK + 2 * HALF
ROW_SCALE = float(np.float32(1.0) / np.sqrt(np.float32(524288.0)))
Z0, CB, X0, Y0 = 0, 2, 3, 5
VMEM = pltpu.VMEM
WHOLE = pl.BlockSpec(memory_space=VMEM)
SMEM = pl.BlockSpec(memory_space=pltpu.SMEM)


def room(mib):
    return pltpu.CompilerParams(vmem_limit_bytes=mib << 20)


def on_chip(values):
    return [pltpu.with_memory_space_constraint(v, pltpu.VMEM) for v in values]


def np_hadamard(order):
    ids = np.arange(order)
    both = ids[:, None] & ids[None, :]
    parity = np.zeros_like(both)
    for offset in range(order.bit_length()):
        parity ^= both >> offset & 1
    return 1 - 2 * parity


def to_partner(value, axis, delta):
    if axis == "z":
        return lax.ppermute(value, "grp", [(i, i ^ delta) for i in range(4)])
    step = {"c": delta, "x": delta << 1, "y": delta << 3}[axis]
    return lax.ppermute(value, "tm", [(i, i ^ step) for i in range(32)])


def prepare_kernel(ids_ref, taps_ref, flips_ref, band_ref, flip_ref):
    for r in range(0, BLK, 32):
        offset = lax.broadcasted_iota(jnp.int32, (32, WIN), 1) - (
            lax.broadcasted_iota(jnp.int32, (32, WIN), 0) + r
        )
        band = jnp.zeros((32, WIN), F32)
        for k in range(TAPS):
            band = jnp.where(offset == k, taps_ref[k], band)
        high = band.astype(BF16)
        low = (band - high.astype(F32)).astype(BF16)
        band_ref[r : r + 32, :] = jnp.concatenate([high, high, low], 1)
    times = lax.broadcasted_iota(jnp.int32, (16, 128), 0) * BLK + lax.broadcasted_iota(
        jnp.int32, (16, 128), 1
    )
    for h in range(2):
        both = (times + 128 * h) & (ids_ref[3] * 32)
        for shift in (8, 4, 2, 1):
            both = both ^ lax.shift_right_logical(both, shift)
        signs = flips_ref[pl.ds(h, 16, stride=2), :] * (1 - 2 * (both & 1))
        flip_ref[:, 128 * h : 128 * h + 128] = signs.astype(F32)


def owners_kernel(ids_ref, samples_ref, a_ref, b_ref, turn_ref):
    yx, core, z = ids_ref[0], ids_ref[1], ids_ref[2]

    def turned(block, half, slot):
        line = lax.shift_right_logical(samples_ref[pl.ds(block * 2 + half, 1), :], 12).astype(F32)
        turn_ref[slot] = jnp.broadcast_to(line, (128, 128)).T

    def column(slot, s, low):
        return turn_ref[slot, pl.ds(low * 64 + s, 32, stride=2), :].astype(jnp.int32)

    for y in range(4):
        for c in range(2):
            for x in range(4):
                turned((yx ^ (y * 4 + x)) * 2 + (core ^ c), z // 2, x)
                for s in range(2):
                    a_ref[s, y, x, c] = jnp.where(z % 2 == 1, column(x, s, 1), column(x, s, 0))
            for h in range(2):
                turned((yx ^ (y * 4)) * 2 + (core ^ c), h, 4 + h)
                for s in range(2):
                    for low in range(2):
                        b_ref[s, y, c, z ^ (2 * h + low)] = column(4 + h, s, low)


def local_kernel(half, x_ref, prev_ref, next_ref, band_ref, had_ref, flip_ref, *refs):
    outs, mid_ref = refs[:4], refs[4]
    cols = slice(256 * half, 256 * half + 256)
    for b in range(16):
        if b == 0:
            window = jnp.concatenate([prev_ref[:, cols], x_ref[0 : BLK + HALF]], 0)
        elif b == 15:
            window = jnp.concatenate([x_ref[b * BLK - HALF :], next_ref[:, cols]], 0)
        else:
            window = x_ref[b * BLK - HALF : (b + 1) * BLK + HALF]
        high = window.astype(BF16)
        low = (window - high.astype(F32)).astype(BF16)
        stacked = jnp.concatenate([high, low, high], 0)
        mid_ref[b] = jnp.dot(band_ref[...], stacked, preferred_element_type=F32)
    for b in range(16):
        filtered = mid_ref[b]
        f_high = filtered.astype(BF16)
        f_low = (filtered - f_high.astype(F32)).astype(BF16)
        signed = had_ref[...] * flip_ref[b : b + 1, :].astype(BF16)
        mid_ref[b] = jnp.dot(
            jnp.concatenate([signed, signed], 1),
            jnp.concatenate([f_high, f_low], 0),
            preferred_element_type=F32,
        )

    def butterflies(at):
        vals = [mid_ref[b, pl.ds(at, 8), :] for b in range(16)]
        for half in (8, 4, 2, 1):
            vals = [
                vals[i] + vals[i + half] if not i & half else vals[i - half] - vals[i]
                for i in range(16)
            ]
        return vals

    def rows_of_z(d, r, _):
        core, part = r // 4, r % 4
        vals = butterflies(pl.multiple_of(core * 128 + d * 32 + part * 8, 8))
        for i in range(16):
            outs[d][i, pl.ds(pl.multiple_of(r * 8, 8), 8), :] = vals[i]
        return 0

    def rows_all(r, _):
        at = pl.multiple_of(r * 8, 8)
        vals = butterflies(at)
        for i in range(16):
            outs[i % 4][i // 4, pl.ds(at, 8), :] = vals[i]
        return 0

    if half == 0:
        for d in range(4):
            lax.fori_loop(0, 8, functools.partial(rows_of_z, d), 0)
    else:
        lax.fori_loop(0, 32, rows_all, 0)


def sign_of(owner, bit, width):
    e = (1 - 2 * (lax.shift_right_logical(owner, bit) & 1)).astype(F32)
    return jnp.concatenate([e] * (width // 128), -1) if width > 128 else e


def core_kernel(pick, keep_ref, recv_ref, o_ref, *outs):
    for s in range(2):
        for y in range(4):
            for d in range(4):
                e = sign_of(o_ref[(s, y, *pick(d))], CB, 256)
                outs[y][s, d] = keep_ref[s, y, d] + e * recv_ref[s, y, d]


def core_stage(keep, recv, owners, pick):
    return pl.pallas_call(
        functools.partial(core_kernel, pick),
        in_specs=[WHOLE] * 3,
        out_specs=[WHOLE] * 4,
        out_shape=[VMEM((2, 4, 32, 256), F32)] * 4,
        compiler_params=room(12),
    )(*on_chip([keep, recv]), owners)


def merged(parts, owner, bit):
    width = parts[0].shape[-1]
    e0, e1 = sign_of(owner, bit, width), sign_of(owner, bit + 1, width)
    return (parts[0] + e0 * parts[1]) + e1 * (parts[2] + e0 * parts[3])


def merge_kernel(bit, cut, pick, *refs):
    ins, o_ref, outs = refs[:4], refs[4], refs[5:]
    lead = ins[0].shape[1:-2]
    for s in range(2):
        for at in np.ndindex(*lead):
            value = merged([r[(s, *at)] for r in ins], o_ref[(s, *pick(*at))], bit)
            rest = tuple(v for d, v in enumerate(at) if d != cut)
            outs[at[cut]][(s, *rest)] = value


def merge_stage(parts, owners, bit, cut, pick):
    shape = parts[0].shape
    out = tuple(v for d, v in enumerate(shape) if d != cut + 1)
    return pl.pallas_call(
        functools.partial(merge_kernel, bit, cut, pick),
        in_specs=[WHOLE] * 5,
        out_specs=[WHOLE] * 4,
        out_shape=[VMEM(out, F32)] * 4,
        compiler_params=room(12),
    )(*on_chip(parts), owners)


def first_kernel(bit, core_dim, *refs):
    ins, o_ref, outs = refs[:4], refs[4], refs[5:]
    for at in np.ndindex(*ins[0].shape[:-2]):
        parts = [r[at] for r in ins]
        rest = tuple(v for d, v in enumerate(at) if d != core_dim)
        for s in range(2):
            outs[at[core_dim]][(s, *rest)] = merged(parts, o_ref[(s, *at)], bit)


def first_stage(parts, owners, bit, core_dim):
    return pl.pallas_call(
        functools.partial(first_kernel, bit, core_dim),
        in_specs=[WHOLE] * 5,
        out_specs=[WHOLE] * 2,
        out_shape=[VMEM((2, 4, 4, 32, 256), F32)] * 2,
        compiler_params=room(12),
    )(*on_chip(parts), owners)


def final_kernel(ids_ref, *refs):
    a_in, b_in = refs[0:4], refs[4:8]
    o_ref, sketch_ref, keep_ref, send_ref, gram_ref = refs[8:]
    core, z, me = ids_ref[1], ids_ref[2], ids_ref[3]
    halves = []
    for s in range(2):
        owner = o_ref[s, 0, 0, 0]
        parity = owner & me
        parity = parity ^ lax.shift_right_logical(parity, 4)
        parity = parity ^ lax.shift_right_logical(parity, 2)
        parity = parity ^ lax.shift_right_logical(parity, 1)
        factor = (1 - 2 * (parity & 1)).astype(F32) * ROW_SCALE
        left = merged([r[s] for r in a_in], owner, X0)
        right = merged([r[s] for r in b_in], owner, Z0)
        rows = jnp.concatenate([left, right], 1) * jnp.concatenate([factor] * 4, 1)
        sketch_ref[:, s, :] = rows
        halves.append(rows)
    both = jnp.concatenate(halves, 0)
    gram_ref[...] = lax.dot_general(
        both, both, (((0,), (0,)), ((), ())),
        precision=lax.Precision.HIGHEST, preferred_element_type=F32,
    )
    for d in range(4):
        for ref, slot in ((keep_ref, core * 4 + (z ^ d)), (send_ref, (1 - core) * 4 + (z ^ d))):
            for t in range(3):
                ref[d, :, 128 * t : 128 * t + 128] = gram_ref[gram_block(slot, t)]


def gram_block(slot, t):
    row = pl.multiple_of(slot * 64, 64)
    col = pl.multiple_of(((slot // 2 + t) & 3) * 128, 128)
    return pl.ds(row, 64), pl.ds(col, 128)


def lane(tile, at):
    ids = lax.broadcasted_iota(jnp.int32, (8, 128), 1)
    return jnp.broadcast_to(jnp.sum(jnp.where(ids == at, tile, 0.0), axis=1, keepdims=True), (8, 128))


def sub(tile, at):
    return jnp.broadcast_to(tile[at : at + 1, :], tile.shape)


def wide(tile, width):
    return jnp.concatenate([tile] * (width // 128), 1) if width > 128 else tile


def cholesky_kernel(ids_ref, s0, s1, s2, s3, p_ref, out_ref, g_ref):
    core, z = ids_ref[1], ids_ref[2]
    for d, mine in enumerate((s0, s1, s2, s3)):
        for t in range(3):
            cut = slice(128 * t, 128 * t + 128)
            g_ref[gram_block(core * 4 + (z ^ d), t)] = mine[:, cut] * (1.0 / 8192)
            g_ref[gram_block((1 - core) * 4 + (z ^ d), t)] = p_ref[d, :, cut] * (1.0 / 8192)
    g_ref[0:128, 384:512] = g_ref[384:512, 0:128].T
    below = lax.broadcasted_iota(jnp.int32, (8, 128), 0)
    step = 32
    for base in range(0, COLS, step):
        lead = base // 128 * 128
        off, width = base - lead, COLS - lead
        row8 = lax.broadcasted_iota(jnp.int32, (8, width), 0)
        col8 = lax.broadcasted_iota(jnp.int32, (8, width), 1)
        tiles = [g_ref[base + 8 * p : base + 8 * p + 8, lead:] for p in range(step // 8)]
        done = []
        for p in range(step // 8):
            cols = [[lane(t[:, :128], off + 8 * p + i) for i in range(8)] for t in tiles[p:]]
            pivots = jnp.ones((8, 128), F32)
            for i in range(8):
                pivot = sub(cols[0][i], i)
                pivots = jnp.where(below == i, pivot, pivots)
                inverse = 1.0 / pivot
                line = sub(tiles[p], i)
                factors = [c[i] * inverse for c in cols]
                factors[0] = jnp.where(below > i, factors[0], 0.0)
                for k in range(i + 1, 8):
                    row = sub(cols[0][k], i)
                    for n, c in enumerate(cols):
                        c[k] = c[k] - factors[n] * row
                for n, f in enumerate(factors):
                    tiles[p + n] = tiles[p + n] - wide(f, width) * line
            rows = tiles[p] * wide(lax.rsqrt(pivots), width)
            rows = jnp.where(col8 >= row8 + (off + 8 * p), rows, 0.0)
            at = base + 8 * p
            out_ref[at : at + 8, lead:] = rows
            if lead:
                out_ref[at : at + 8, :lead] = jnp.zeros((8, lead), F32)
            done.append(rows)
        after = base + step
        if after < COLS:
            left = after // 128 * 128
            rows = jnp.concatenate(done, 0)[:, left - lead :]
            one = rows.astype(BF16)
            rest = rows - one.astype(F32)
            two = rest.astype(BF16)
            three = (rest - two.astype(F32)).astype(BF16)
            update = lax.dot_general(
                jnp.concatenate([one, one, two, one, three, two], 0),
                jnp.concatenate([one, two, one, three, one, two], 0),
                (((0,), (0,)), ((), ())), preferred_element_type=F32,
            )
            g_ref[after:, left:] -= update[after - left :, :]


def spread(parts, axis):
    moved = [parts[0]]
    for d in (1, 2, 3):
        moved.append(to_partner(parts[d], axis, d))
    return moved


def summed(value, axis):
    one, two, three = (to_partner(value, axis, d) for d in (1, 2, 3))
    return (value + one) + (two + three)


def on_device(series, filter_taps, sign_flips, samples):
    tm, z = lax.axis_index("tm"), lax.axis_index("grp")
    me = tm * 4 + z
    ids = jnp.stack([tm // 2, tm % 2, z, me]).astype(jnp.int32)

    up = [(i, i + 1) for i in range(127)]
    prev = lax.ppermute(series[ROWS_DEV - HALF :], ("tm", "grp"), up)
    nxt = lax.ppermute(series[:HALF], ("tm", "grp"), [(b, a) for a, b in up])

    had = jnp.asarray(np_hadamard(BLK), BF16)
    bands, flips = pl.pallas_call(
        prepare_kernel,
        in_specs=[SMEM, SMEM, WHOLE],
        out_specs=[WHOLE] * 2,
        out_shape=[VMEM((BLK, 3 * WIN), BF16), VMEM((16, BLK), F32)],
        compiler_params=room(12),
    )(ids, filter_taps, sign_flips.reshape(32, 128))
    prev, nxt, bands, flips = on_chip([prev, nxt, bands, flips])

    firsts = []
    for half in range(2):
        cut = lambda i, half=half: (0, half)
        out = (16, 64, 256) if half == 0 else (4, 256, 256)
        parts = pl.pallas_call(
            functools.partial(local_kernel, half),
            grid=(1,),
            in_specs=[pl.BlockSpec((ROWS_DEV, 256), cut)] + [WHOLE] * 5,
            out_specs=[WHOLE] * 4,
            out_shape=[VMEM(out, F32)] * 4,
            scratch_shapes=[VMEM((16, BLK, 256), F32)],
            compiler_params=room(24),
        )(series, prev, nxt, bands, had, flips)
        shape = (4, 4, 2, 32, 256) if half == 0 else (4, 2, 4, 32, 256)
        firsts.append([p.reshape(shape) for p in parts])

    a = spread(firsts[0], "z")
    b = spread(firsts[1], "x")
    late, b[0] = lax.optimization_barrier((samples.reshape(64, 128), b[0]))
    owners_a, owners_b = pl.pallas_call(
        owners_kernel,
        in_specs=[SMEM, WHOLE],
        out_specs=[WHOLE] * 2,
        out_shape=[VMEM((2, 4, 4, 2, 32, 128), jnp.int32), VMEM((2, 4, 2, 4, 32, 128), jnp.int32)],
        scratch_shapes=[VMEM((6, 128, 128), F32)],
        compiler_params=room(12),
    )(ids, late)

    owners_a, owners_b = on_chip([owners_a, owners_b])
    keep, send = first_stage(a, owners_a, Z0, 2)
    a = list(core_stage(keep, to_partner(send, "c", 1), owners_a, lambda x: (x, 0)))
    a = spread(a, "y")
    keep, send = first_stage(b, owners_b, X0, 1)
    b = core_stage(keep, to_partner(send, "c", 1), owners_b, lambda z: (0, z))
    b = spread(b, "y")
    a = merge_stage(a, owners_a, Y0, 0, lambda x: (0, x, 0))
    a = spread(a, "x")
    b = merge_stage(b, owners_b, Y0, 0, lambda z: (0, 0, z))
    b = spread(b, "z")

    sketch, keep, send = pl.pallas_call(
        final_kernel,
        in_specs=[SMEM] + [WHOLE] * 9,
        out_specs=[WHOLE] * 3,
        out_shape=[
            jax.ShapeDtypeStruct((32, 2, COLS), F32),
            VMEM((4, 64, 384), F32),
            VMEM((4, 64, 384), F32),
        ],
        scratch_shapes=[VMEM((COLS, COLS), F32)],
        compiler_params=room(12),
    )(ids, *on_chip(a), *on_chip(b), owners_a)
    sketch = sketch.reshape(64, COLS)

    held = keep + to_partner(send, "c", 1)
    one, two, three = (to_partner(held[d], "z", d) for d in (1, 2, 3))
    share = (held[0] + one) + (two + three)
    share = summed(share, "x")
    share = summed(share, "y")
    near = [share] + [to_partner(share, "z", d) for d in (1, 2, 3)]
    far = to_partner(jnp.stack(near), "c", 1)

    r_factor = pl.pallas_call(
        cholesky_kernel,
        in_specs=[SMEM] + [WHOLE] * 5,
        out_specs=WHOLE,
        out_shape=jax.ShapeDtypeStruct((COLS, COLS), F32),
        scratch_shapes=[VMEM((COLS, COLS), F32)],
        compiler_params=room(12),
    )(ids, *on_chip(near), *on_chip([far]))
    return (sketch, r_factor)


def solution(mesh):
    return jax.shard_map(
        on_device,
        mesh=mesh,
        in_specs=(P(("tm", "grp"), None), P(), P(("tm", "grp")), P()),
        out_specs=(P(("tm", "grp"), None), P()),
        check_vma=False,
    )
```

```python
import functools

import jax
import jax.numpy as jnp
import numpy as np
from jax import lax
from jax.experimental import pallas as pl
from jax.experimental.pallas import tpu as pltpu
from jax.sharding import PartitionSpec as P


F32 = jnp.float32
BF16 = jnp.bfloat16
ROWS_DEV = 4096
COLS = 512
HALF = 16
TAPS = 33
BLK = 256
WIN = BLK + 2 * HALF
ROW_SCALE = float(np.float32(1.0) / np.sqrt(np.float32(524288.0)))
Z0, CB, X0, Y0 = 0, 2, 3, 5
VMEM = pltpu.VMEM
WHOLE = pl.BlockSpec(memory_space=VMEM)
SMEM = pl.BlockSpec(memory_space=pltpu.SMEM)


def room(mib):
    return pltpu.CompilerParams(vmem_limit_bytes=mib << 20)


def on_chip(values):
    return [pltpu.with_memory_space_constraint(v, pltpu.VMEM) for v in values]


def to_partner(value, axis, delta):
    if axis == "z":
        return lax.ppermute(value, "grp", [(i, i ^ delta) for i in range(4)])
    step = {"c": delta, "x": delta << 1, "y": delta << 3}[axis]
    return lax.ppermute(value, "tm", [(i, i ^ step) for i in range(32)])


def prepare_kernel(ids_ref, taps_ref, flips_ref, band_ref, flip_ref, had_ref):
    for r in range(0, BLK, 32):
        both = (lax.broadcasted_iota(jnp.int32, (32, BLK), 0) + r) & lax.broadcasted_iota(
            jnp.int32, (32, BLK), 1
        )
        for shift in (4, 2, 1):
            both = both ^ lax.shift_right_logical(both, shift)
        had_ref[r : r + 32, :] = (1 - 2 * (both & 1)).astype(F32).astype(BF16)
    for r in range(0, BLK, 32):
        offset = lax.broadcasted_iota(jnp.int32, (32, WIN), 1) - (
            lax.broadcasted_iota(jnp.int32, (32, WIN), 0) + r
        )
        band = jnp.zeros((32, WIN), F32)
        for k in range(TAPS):
            band = jnp.where(offset == k, taps_ref[k], band)
        high = band.astype(BF16)
        low = (band - high.astype(F32)).astype(BF16)
        band_ref[r : r + 32, :] = jnp.concatenate([high, high, low], 1)
    times = lax.broadcasted_iota(jnp.int32, (16, 128), 0) * BLK + lax.broadcasted_iota(
        jnp.int32, (16, 128), 1
    )
    for h in range(2):
        both = (times + 128 * h) & (ids_ref[3] * 32)
        for shift in (8, 4, 2, 1):
            both = both ^ lax.shift_right_logical(both, shift)
        signs = flips_ref[pl.ds(h, 16, stride=2), :] * (1 - 2 * (both & 1))
        flip_ref[:, 128 * h : 128 * h + 128] = signs.astype(F32)


def owners_kernel(ids_ref, samples_ref, a_ref, b_ref, c_ref, turn_ref):
    yx, core, z = ids_ref[0], ids_ref[1], ids_ref[2]

    def turned(block, half, slot):
        line = lax.shift_right_logical(samples_ref[pl.ds(block * 2 + half, 1), :], 12).astype(F32)
        turn_ref[slot] = jnp.broadcast_to(line, (128, 128)).T

    def column(slot, s, low):
        return turn_ref[slot, pl.ds(low * 64 + s, 32, stride=2), :].astype(jnp.int32)

    for y in range(4):
        for c in range(2):
            for x in range(4):
                turned((yx ^ (y * 4 + x)) * 2 + (core ^ c), z // 2, x)
                for s in range(2):
                    a_ref[s, y, x, c] = jnp.where(z % 2 == 1, column(x, s, 1), column(x, s, 0))
            for h in range(2):
                turned((yx ^ (y * 4)) * 2 + (core ^ c), h, 4 + h)
                for s in range(2):
                    for low in range(2):
                        b_ref[s, y, c, z ^ (2 * h + low)] = column(4 + h, s, low)
                turned((yx ^ y) * 2 + (core ^ c), h, 6 + h)
                for s in range(2):
                    for low in range(2):
                        c_ref[s, y, c, z ^ (2 * h + low)] = column(6 + h, s, low)[24:32]


def local_kernel(half, x_ref, prev_ref, next_ref, band_ref, had_ref, flip_ref, *refs):
    outs, (mid_ref, rows_ref, arrived) = refs[:-3], refs[-3:]
    cols = slice(256 * half, 256 * half + 256)
    step = ROWS_DEV // 4
    copies = [
        pltpu.make_async_copy(x_ref.at[step * j : step * j + step, cols], rows_ref.at[step * j : step * j + step], arrived.at[j])
        for j in range(4)
    ]
    for copy in copies:
        copy.start()
    waited = 0
    for b in range(16):
        while waited < 4 and waited * step < (b + 1) * BLK + HALF:
            copies[waited].wait()
            waited += 1
        if b == 0:
            window = jnp.concatenate([prev_ref[:, cols], rows_ref[0 : BLK + HALF]], 0)
        elif b == 15:
            window = jnp.concatenate([rows_ref[b * BLK - HALF :], next_ref[:, cols]], 0)
        else:
            window = rows_ref[b * BLK - HALF : (b + 1) * BLK + HALF]
        high = window.astype(BF16)
        low = (window - high.astype(F32)).astype(BF16)
        stacked = jnp.concatenate([high, low, high], 0)
        mid_ref[b] = jnp.dot(band_ref[...], stacked, preferred_element_type=F32)
    for b in range(16):
        filtered = mid_ref[b]
        f_high = filtered.astype(BF16)
        f_low = (filtered - f_high.astype(F32)).astype(BF16)
        signed = had_ref[...] * flip_ref[b : b + 1, :].astype(BF16)
        mid_ref[b] = jnp.dot(
            jnp.concatenate([signed, signed], 1),
            jnp.concatenate([f_high, f_low], 0),
            preferred_element_type=F32,
        )

    def butterflies(at):
        vals = [mid_ref[b, pl.ds(at, 8), :] for b in range(16)]
        for half in (8, 4, 2, 1):
            vals = [
                vals[i] + vals[i + half] if not i & half else vals[i - half] - vals[i]
                for i in range(16)
            ]
        return vals

    def rows_of_z(d, r, _):
        core, part = r // 4, r % 4
        vals = butterflies(pl.multiple_of(core * 128 + d * 32 + part * 8, 8))
        for i in range(16):
            outs[d][i, pl.ds(pl.multiple_of(r * 8, 8), 8), :] = vals[i]
        return 0

    def rows_split(r, _):
        for part in range(4):
            vals = butterflies(pl.multiple_of(r * 32 + part * 8, 8))
            for i in range(16):
                if part < 3:
                    at = pl.multiple_of(r * 24 + part * 8, 8)
                    outs[i % 4][i // 4, pl.ds(at, 8), :] = vals[i]
                else:
                    outs[4 + i // 4][i % 4, pl.ds(pl.multiple_of(r * 8, 8), 8), :] = vals[i]
        return 0

    if half == 0:
        for d in range(4):
            lax.fori_loop(0, 8, functools.partial(rows_of_z, d), 0)
    else:
        lax.fori_loop(0, 8, rows_split, 0)


def sign_of(owner, bit, width):
    e = (1 - 2 * (lax.shift_right_logical(owner, bit) & 1)).astype(F32)
    return jnp.concatenate([e] * (width // 128), -1) if width > 128 else e


def core_kernel(cut, pick, keep_ref, recv_ref, o_ref, *outs):
    for s in range(2):
        for at in np.ndindex(4, 4):
            e = sign_of(o_ref[(s, *pick(*at), slice(0, keep_ref.shape[-2]))], CB, 256)
            outs[at[cut]][s, at[1 - cut]] = keep_ref[(s, *at)] + e * recv_ref[(s, *at)]


def core_stage(keep, recv, owners, cut, pick):
    return pl.pallas_call(
        functools.partial(core_kernel, cut, pick),
        in_specs=[WHOLE] * 3,
        out_specs=[WHOLE] * 4,
        out_shape=[VMEM((2, 4, *keep.shape[-2:]), F32)] * 4,
        compiler_params=room(12),
    )(*on_chip([keep, recv]), owners)


def merged(parts, owner, bit):
    width = parts[0].shape[-1]
    e0, e1 = sign_of(owner, bit, width), sign_of(owner, bit + 1, width)
    return (parts[0] + e0 * parts[1]) + e1 * (parts[2] + e0 * parts[3])


def merge_kernel(bit, cut, pick, *refs):
    ins, o_ref, outs = refs[:4], refs[4], refs[5:]
    lead = ins[0].shape[1:-2]
    for s in range(2):
        for at in np.ndindex(*lead):
            owner = o_ref[(s, *pick(*at), slice(0, ins[0].shape[-2]))]
            value = merged([r[(s, *at)] for r in ins], owner, bit)
            rest = tuple(v for d, v in enumerate(at) if d != cut)
            outs[at[cut]][(s, *rest)] = value


def merge_stage(parts, owners, bit, cut, pick):
    shape = parts[0].shape
    out = tuple(v for d, v in enumerate(shape) if d != cut + 1)
    return pl.pallas_call(
        functools.partial(merge_kernel, bit, cut, pick),
        in_specs=[WHOLE] * 5,
        out_specs=[WHOLE] * 4,
        out_shape=[VMEM(out, F32)] * 4,
        compiler_params=room(12),
    )(*on_chip(parts), owners)


def first_kernel(bit, core_dim, *refs):
    ins, o_ref, outs = refs[:4], refs[4], refs[5:]
    for at in np.ndindex(*ins[0].shape[:-2]):
        parts = [r[at] for r in ins]
        rest = tuple(v for d, v in enumerate(at) if d != core_dim)
        for s in range(2):
            owner = o_ref[(s, *at, slice(0, parts[0].shape[-2]))]
            outs[at[core_dim]][(s, *rest)] = merged(parts, owner, bit)


def first_stage(parts, owners, bit, core_dim):
    return pl.pallas_call(
        functools.partial(first_kernel, bit, core_dim),
        in_specs=[WHOLE] * 5,
        out_specs=[WHOLE] * 2,
        out_shape=[VMEM((2, 4, 4, *parts[0].shape[-2:]), F32)] * 2,
        compiler_params=room(12),
    )(*on_chip(parts), owners)


def final_kernel(ids_ref, *refs):
    a_in, b_in, c_in = refs[0:4], refs[4:8], refs[8:12]
    o_ref, sketch_ref, keep_ref, send_ref, gram_ref = refs[12:]
    core, z, me = ids_ref[1], ids_ref[2], ids_ref[3]
    halves = []
    for s in range(2):
        owner = o_ref[s, 0, 0, 0]
        parity = owner & me
        parity = parity ^ lax.shift_right_logical(parity, 4)
        parity = parity ^ lax.shift_right_logical(parity, 2)
        parity = parity ^ lax.shift_right_logical(parity, 1)
        factor = (1 - 2 * (parity & 1)).astype(F32) * ROW_SCALE
        left = merged([r[s] for r in a_in], owner, X0)
        upper = merged([r[s] for r in b_in], owner[0:24], Y0)
        lower = merged([r[s] for r in c_in], owner[24:32], X0)
        right = jnp.concatenate([upper, lower], 0)
        rows = jnp.concatenate([left, right], 1) * jnp.concatenate([factor] * 4, 1)
        sketch_ref[:, s, :] = rows
        halves.append(rows)
    both = jnp.concatenate(halves, 0)
    gram_ref[...] = lax.dot_general(
        both, both, (((0,), (0,)), ((), ())),
        precision=lax.Precision.HIGHEST, preferred_element_type=F32,
    )
    for d in range(4):
        for ref, slot in ((keep_ref, core * 4 + (z ^ d)), (send_ref, (1 - core) * 4 + (z ^ d))):
            for t in range(3):
                ref[d, :, 128 * t : 128 * t + 128] = gram_ref[gram_block(slot, t)]


def gram_block(slot, t):
    row = pl.multiple_of(slot * 64, 64)
    col = pl.multiple_of(((slot // 2 + t) & 3) * 128, 128)
    return pl.ds(row, 64), pl.ds(col, 128)


def lane(tile, at):
    ids = lax.broadcasted_iota(jnp.int32, (8, 128), 1)
    return jnp.broadcast_to(jnp.sum(jnp.where(ids == at, tile, 0.0), axis=1, keepdims=True), (8, 128))


def sub(tile, at):
    return jnp.broadcast_to(tile[at : at + 1, :], tile.shape)


def wide(tile, width):
    return jnp.concatenate([tile] * (width // 128), 1) if width > 128 else tile


def cholesky_kernel(ids_ref, s0, s1, s2, s3, p_ref, out_ref, g_ref):
    core, z = ids_ref[1], ids_ref[2]
    for d, mine in enumerate((s0, s1, s2, s3)):
        for t in range(3):
            cut = slice(128 * t, 128 * t + 128)
            g_ref[gram_block(core * 4 + (z ^ d), t)] = mine[:, cut] * (1.0 / 8192)
            g_ref[gram_block((1 - core) * 4 + (z ^ d), t)] = p_ref[d, :, cut] * (1.0 / 8192)
    g_ref[0:128, 384:512] = g_ref[384:512, 0:128].T
    below = lax.broadcasted_iota(jnp.int32, (8, 128), 0)
    step = 32
    for base in range(0, COLS, step):
        lead = base // 128 * 128
        off, width = base - lead, COLS - lead
        row8 = lax.broadcasted_iota(jnp.int32, (8, width), 0)
        col8 = lax.broadcasted_iota(jnp.int32, (8, width), 1)
        tiles = [g_ref[base + 8 * p : base + 8 * p + 8, lead:] for p in range(step // 8)]
        done = []
        for p in range(step // 8):
            cols = [[lane(t[:, :128], off + 8 * p + i) for i in range(8)] for t in tiles[p:]]
            pivots = jnp.ones((8, 128), F32)
            for i in range(8):
                pivot = sub(cols[0][i], i)
                pivots = jnp.where(below == i, pivot, pivots)
                inverse = 1.0 / pivot
                line = sub(tiles[p], i)
                factors = [c[i] * inverse for c in cols]
                factors[0] = jnp.where(below > i, factors[0], 0.0)
                for k in range(i + 1, 8):
                    row = sub(cols[0][k], i)
                    for n, c in enumerate(cols):
                        c[k] = c[k] - factors[n] * row
                for n, f in enumerate(factors):
                    tiles[p + n] = tiles[p + n] - wide(f, width) * line
            rows = tiles[p] * wide(lax.rsqrt(pivots), width)
            rows = jnp.where(col8 >= row8 + (off + 8 * p), rows, 0.0)
            at = base + 8 * p
            out_ref[at : at + 8, lead:] = rows
            if lead:
                out_ref[at : at + 8, :lead] = jnp.zeros((8, lead), F32)
            done.append(rows)
        after = base + step
        if after < COLS:
            left = after // 128 * 128
            rows = jnp.concatenate(done, 0)[:, left - lead :]
            one = rows.astype(BF16)
            rest = rows - one.astype(F32)
            two = rest.astype(BF16)
            three = (rest - two.astype(F32)).astype(BF16)
            update = lax.dot_general(
                jnp.concatenate([one, one, two, one, three, two], 0),
                jnp.concatenate([one, two, one, three, one, two], 0),
                (((0,), (0,)), ((), ())), preferred_element_type=F32,
            )
            g_ref[after:, left:] -= update[after - left :, :]


def spread(parts, axis):
    moved = [parts[0]]
    for d in (1, 2, 3):
        moved.append(to_partner(parts[d], axis, d))
    return moved


def summed(values, axis):
    own, one, two, three = spread(values, axis)
    return (own + one) + (two + three)


def on_device(series, filter_taps, sign_flips, samples):
    tm, z = lax.axis_index("tm"), lax.axis_index("grp")
    me = tm * 4 + z
    ids = jnp.stack([tm // 2, tm % 2, z, me]).astype(jnp.int32)

    up = [(i, i + 1) for i in range(127)]
    prev = lax.ppermute(series[ROWS_DEV - HALF :], ("tm", "grp"), up)
    nxt = lax.ppermute(series[:HALF], ("tm", "grp"), [(b, a) for a, b in up])

    bands, flips, had = pl.pallas_call(
        prepare_kernel,
        in_specs=[SMEM, SMEM, WHOLE],
        out_specs=[WHOLE] * 3,
        out_shape=[VMEM((BLK, 3 * WIN), BF16), VMEM((16, BLK), F32), VMEM((BLK, BLK), BF16)],
        compiler_params=room(12),
    )(ids, filter_taps, sign_flips.reshape(32, 128))
    prev, nxt, bands, flips, had = on_chip([prev, nxt, bands, flips, had])

    rows = pltpu.with_memory_space_constraint(series, pltpu.HBM)
    firsts = []
    for half in range(2):
        outs = [(16, 64, 256)] * 4 if half == 0 else [(4, 192, 256)] * 4 + [(4, 64, 256)] * 4
        parts = pl.pallas_call(
            functools.partial(local_kernel, half),
            in_specs=[pl.BlockSpec(memory_space=pl.ANY)] + [WHOLE] * 5,
            out_specs=[WHOLE] * len(outs),
            out_shape=[VMEM(out, F32) for out in outs],
            scratch_shapes=[
                VMEM((16, BLK, 256), F32),
                VMEM((ROWS_DEV, 256), F32),
                pltpu.SemaphoreType.DMA((4,)),
            ],
            compiler_params=room(24),
        )(rows, prev, nxt, bands, had, flips)
        if half == 0:
            firsts.append([p.reshape(4, 4, 2, 32, 256) for p in parts])
        else:
            firsts.append([p.reshape(4, 2, 4, 24, 256) for p in parts[:4]])
            firsts.append([p.reshape(4, 2, 4, 8, 256) for p in parts[4:]])

    a = spread(firsts[0], "z")
    b = spread(firsts[1], "x")
    c = spread(firsts[2], "y")
    late, b[0] = lax.optimization_barrier((samples.reshape(64, 128), b[0]))
    owners_a, owners_b, owners_c = pl.pallas_call(
        owners_kernel,
        in_specs=[SMEM, WHOLE],
        out_specs=[WHOLE] * 3,
        out_shape=[VMEM((2, 4, 4, 2, 32, 128), jnp.int32), VMEM((2, 4, 2, 4, 32, 128), jnp.int32), VMEM((2, 4, 2, 4, 8, 128), jnp.int32)],
        scratch_shapes=[VMEM((8, 128, 128), F32)],
        compiler_params=room(12),
    )(ids, late)

    owners_a, owners_b, owners_c = on_chip([owners_a, owners_b, owners_c])
    keep, send = first_stage(c, owners_c, Y0, 1)
    c = core_stage(keep, to_partner(send, "c", 1), owners_c, 1, lambda x, z: (x, 0, z))
    c = spread(c, "z")
    c = merge_stage(c, owners_c, Z0, 0, lambda x: (x, 0, 0))
    c = spread(c, "x")
    keep, send = first_stage(a, owners_a, Z0, 2)
    moved = to_partner(send, "c", 1)
    a = core_stage(keep, moved, owners_a, 0, lambda y, x: (y, x, 0))
    a = spread(a, "y")
    keep, send = first_stage(b, owners_b, X0, 1)
    b = core_stage(keep, to_partner(send, "c", 1), owners_b, 1, lambda y, z: (y, 0, z))
    b = spread(b, "z")
    a = merge_stage(a, owners_a, Y0, 0, lambda x: (0, x, 0))
    a = spread(a, "x")
    b = merge_stage(b, owners_b, Z0, 0, lambda y: (y, 0, 0))
    b = spread(b, "y")

    sketch, keep, send = pl.pallas_call(
        final_kernel,
        in_specs=[SMEM] + [WHOLE] * 13,
        out_specs=[WHOLE] * 3,
        out_shape=[
            jax.ShapeDtypeStruct((32, 2, COLS), F32),
            VMEM((4, 64, 384), F32),
            VMEM((4, 64, 384), F32),
        ],
        scratch_shapes=[VMEM((COLS, COLS), F32)],
        compiler_params=room(12),
    )(ids, *on_chip(a), *on_chip(b), *on_chip(c), owners_a)
    sketch = sketch.reshape(64, COLS)

    held = keep + to_partner(send, "c", 1)
    share = summed(held, "z")
    share = summed([share] * 4, "x")
    share = summed([share] * 4, "y")
    near = spread([share] * 4, "z")
    far = to_partner(jnp.stack(near), "c", 1)

    r_factor = pl.pallas_call(
        cholesky_kernel,
        in_specs=[SMEM] + [WHOLE] * 5,
        out_specs=WHOLE,
        out_shape=jax.ShapeDtypeStruct((COLS, COLS), F32),
        scratch_shapes=[VMEM((COLS, COLS), F32)],
        compiler_params=room(12),
    )(ids, *on_chip(near), *on_chip([far]))
    return (sketch, r_factor)


def solution(mesh):
    return jax.shard_map(
        on_device,
        mesh=mesh,
        in_specs=(P(("tm", "grp"), None), P(), P(("tm", "grp")), P()),
        out_specs=(P(("tm", "grp"), None), P()),
        check_vma=False,
    )
```
